8 devices in a mesh: data: 1 (over z), cp: 2 (over y), tp: 4 (over x, core).
Axes of the slice: x: 2, y: 2, z: 1, core: 2. Of those that a mesh axis runs over, the one named last changes fastest.
Arguments:
- x_in: bfloat16 [4096, 2048], P(('data', 'cp', 'tp'))
- w_q: bfloat16 [2048, 32, 128], P(None, 'tp')
- w_k: bfloat16 [2048, 4, 128], P(None, 'tp')
- w_v: bfloat16 [2048, 4, 128], P(None, 'tp')
- w_o: bfloat16 [32, 128, 2048], P('tp')
- expert_idx: int32 [4096, 2], P(('data', 'cp', 'tp'))
- gate_wts: float32 [4096, 2], P(('data', 'cp', 'tp'))
- w_gate: bfloat16 [128, 2048, 768], P(('cp', 'tp'))
- w_up: bfloat16 [128, 2048, 768], P(('cp', 'tp'))
- w_down: bfloat16 [128, 768, 2048], P(('cp', 'tp'))
Outputs:
- output: bfloat16 [4096, 2048], P(('data', 'cp', 'tp'))
All inputs are finite; a program needn't handle non-finite values.
Results may differ from the reference program's by a relative error of at most 0.0146991.
Values are sent between devices in bfloat16 or wider.
A program may use at most 1 GiB of HBM per device.

```python
import math
import jax
import jax.numpy as jnp
import numpy as np
from jax import lax

D = 2048
FF = 768
HEADS = 32
KV_HEADS = 4
HEAD = 128
EXPERTS = 128
TOK_DEV = 512
CP_SIZE = 2
TP_SIZE = 4

NUM_DEVS = CP_SIZE * TP_SIZE
SEQ_LEN = TOK_DEV * NUM_DEVS
HALF_ROWS = TOK_DEV // 2
SEG_LEN = HALF_ROWS * TP_SIZE
CAPACITY = 4 * TOK_DEV // EXPERTS
Q_PER_KV = HEADS // KV_HEADS


def draw_routing(key):
    key_hot, key_src = jax.random.split(key)
    rest_cnt = 2 * TOK_DEV - 2 * CAPACITY
    base_cnt, extra_cnt = divmod(rest_cnt, EXPERTS - 2)
    counts = [CAPACITY, CAPACITY] + [base_cnt + 1] * extra_cnt + [base_cnt] * (EXPERTS - 2 - extra_cnt)
    rank_table = np.repeat(np.arange(EXPERTS), counts)
    rank_ids = jnp.asarray(rank_table).astype(jnp.int32)
    hot_pair = jnp.asarray(rank_table[:TOK_DEV] < 2).astype(jnp.int32)
    expert_perm = jax.random.permutation(key_hot, EXPERTS)

    def one_source(src_dev):
        key_perm, key_rank, key_swap = jax.random.split(jax.random.fold_in(key_src, src_dev), 3)
        cold_ids = expert_perm[2:][jax.random.permutation(key_perm, EXPERTS - 2)]
        id_table = jnp.concatenate([expert_perm[:2], cold_ids])
        choice_ids = id_table[rank_ids]
        rand_rank = jax.random.permutation(key_rank, TOK_DEV)
        pair_score = (rand_rank + hot_pair * (TOK_DEV // 2)) * TOK_DEV + rand_rank
        pair_order = jnp.argsort(pair_score)
        first_ids = choice_ids[:TOK_DEV][pair_order]
        second = choice_ids[TOK_DEV:][pair_order]
        swap_flag = jax.random.randint(key_swap, (TOK_DEV,), 0, 2) == 1
        return jnp.stack([jnp.where(swap_flag, second, first_ids), jnp.where(swap_flag, first_ids, second)], axis=1)

    return jax.vmap(one_source)(jnp.arange(NUM_DEVS)).reshape(SEQ_LEN, 2).astype(jnp.int32)


def row_positions():
    rows_all = jnp.arange(SEQ_LEN)
    dev_index = rows_all // TOK_DEV
    cp_rank = dev_index // TP_SIZE
    tp_rank = dev_index % TP_SIZE
    within = rows_all % TOK_DEV
    seg_index = jnp.where(within < HALF_ROWS, cp_rank, 2 * CP_SIZE - 1 - cp_rank)
    return seg_index * SEG_LEN + tp_rank * HALF_ROWS + within % HALF_ROWS


def setup_inputs(seed: int = 0, part: int = 0) -> dict:
    key_q, key_k, key_v, key_o, key_g, key_u, key_d = jax.random.split(jax.random.key(seed), 7)
    key_x, key_route, key_gate = jax.random.split(jax.random.fold_in(jax.random.key(seed + 1), part), 3)
    score_gain = math.sqrt(0.8 * math.log(SEQ_LEN))
    x_in = jax.random.normal(key_x, (SEQ_LEN, D), jnp.float32)
    w_q = jax.random.normal(key_q, (D, HEADS, HEAD), jnp.float32) * (score_gain / math.sqrt(D))
    w_k = jax.random.normal(key_k, (D, KV_HEADS, HEAD), jnp.float32) / math.sqrt(D)
    w_v = jax.random.normal(key_v, (D, KV_HEADS, HEAD), jnp.float32) / math.sqrt(D)
    w_o = jax.random.normal(key_o, (HEADS, HEAD, D), jnp.float32) / math.sqrt(HEADS * HEAD)
    w_gate = jax.random.normal(key_g, (EXPERTS, D, FF), jnp.float32) / math.sqrt(D)
    w_up = jax.random.normal(key_u, (EXPERTS, D, FF), jnp.float32) / math.sqrt(D)
    w_down = jax.random.normal(key_d, (EXPERTS, FF, D), jnp.float32) * (1.5 / math.sqrt(FF))
    gate_wts = jax.random.uniform(key_gate, (SEQ_LEN, 2), jnp.float32, 0.3, 0.7)
    return {'x_in': x_in.astype(jnp.bfloat16), 'w_q': w_q.astype(jnp.bfloat16), 'w_k': w_k.astype(jnp.bfloat16), 'w_v': w_v.astype(jnp.bfloat16), 'w_o': w_o.astype(jnp.bfloat16), 'expert_idx': draw_routing(key_route), 'gate_wts': gate_wts, 'w_gate': w_gate.astype(jnp.bfloat16), 'w_up': w_up.astype(jnp.bfloat16), 'w_down': w_down.astype(jnp.bfloat16)}


def reference(x_in, w_q, w_k, w_v, w_o, expert_idx, gate_wts, w_gate, w_up, w_down):
    positions = row_positions()
    queries = jnp.dot(x_in, w_q.reshape(D, HEADS * HEAD), preferred_element_type=jnp.float32).astype(jnp.bfloat16)
    keys_all = jnp.dot(x_in, w_k.reshape(D, KV_HEADS * HEAD), preferred_element_type=jnp.float32).astype(jnp.bfloat16)
    keys_all = keys_all.reshape(SEQ_LEN, KV_HEADS, HEAD).astype(jnp.float32)
    values_all = jnp.dot(x_in, w_v.reshape(D, KV_HEADS * HEAD), preferred_element_type=jnp.float32).astype(jnp.bfloat16)
    values_all = values_all.reshape(SEQ_LEN, KV_HEADS, HEAD).astype(jnp.float32)
    att_scale = 1.0 / math.sqrt(HEAD)

    def attend(q_inputs):
        q_block, q_pos = q_inputs
        scores = jnp.einsum('qngc,knc->ngqk', q_block.astype(jnp.float32), keys_all) * att_scale
        scores = jnp.where(positions[None, None, None, :] <= q_pos[None, None, :, None], scores, -jnp.inf)
        exp_scores = jnp.exp(scores - jnp.max(scores, axis=-1, keepdims=True))
        attn_prob = (exp_scores / jnp.sum(exp_scores, axis=-1, keepdims=True)).astype(jnp.bfloat16)
        head_out = jnp.einsum('ngqk,knc->qngc', attn_prob.astype(jnp.float32), values_all)
        return head_out.astype(jnp.bfloat16).reshape(TOK_DEV, HEADS * HEAD)

    head_rows = lax.map(attend, (queries.reshape(NUM_DEVS, TOK_DEV, KV_HEADS, Q_PER_KV, HEAD), positions.reshape(NUM_DEVS, TOK_DEV)))
    attn_out = jnp.dot(head_rows.reshape(SEQ_LEN, HEADS * HEAD), w_o.reshape(HEADS * HEAD, D), preferred_element_type=jnp.float32)
    hidden = (x_in.astype(jnp.float32) + attn_out).astype(jnp.bfloat16)

    flat_ids = expert_idx.reshape(NUM_DEVS, 2 * TOK_DEV)
    onehot = (flat_ids[:, :, None] == jnp.arange(EXPERTS)[None, None, :]).astype(jnp.int32)
    slot_pos = jnp.sum(jnp.cumsum(onehot, axis=1) * onehot, axis=2) - 1
    source = jnp.arange(NUM_DEVS)[:, None]
    dest_row = ((flat_ids * NUM_DEVS + source) * CAPACITY + slot_pos).reshape(-1)
    buffer = jnp.zeros((EXPERTS * NUM_DEVS * CAPACITY, D), jnp.bfloat16).at[dest_row].set(jnp.repeat(hidden, 2, axis=0))

    def expert_ffn(expert_in):
        tok_rows, gate_w, up_w, down_w = expert_in
        gate_pre = jnp.dot(tok_rows, gate_w, preferred_element_type=jnp.float32)
        up_pre = jnp.dot(tok_rows, up_w, preferred_element_type=jnp.float32)
        hid_act = (jax.nn.silu(gate_pre) * up_pre).astype(jnp.bfloat16)
        return jnp.dot(hid_act, down_w, preferred_element_type=jnp.float32).astype(jnp.bfloat16)

    expert_out = lax.map(expert_ffn, (buffer.reshape(EXPERTS, NUM_DEVS * CAPACITY, D), w_gate, w_up, w_down))
    picked = expert_out.reshape(-1, D)[dest_row].reshape(SEQ_LEN, 2, D).astype(jnp.float32)
    moe_out = jnp.sum(gate_wts[:, :, None] * picked, axis=1)
    return (hidden.astype(jnp.float32) + moe_out).astype(jnp.bfloat16)
```

```python
import functools
import jax
import jax.numpy as jnp
from jax import lax
from jax.experimental import pallas as pl
from jax.experimental.pallas import tpu as pltpu
from jax.sharding import PartitionSpec as P

QB = 256
KB = 512
LOG2E = 1.4426950408889634
VLIM = 62 * 1024 * 1024


def attend_block(q_of, k_ref, v_ref, m_ref, l_ref, acc_ref, pos0, heads, hd):
    c = (hd ** -0.5) * LOG2E
    m_ref[...] = jnp.full(m_ref.shape, -jnp.inf, jnp.float32)
    l_ref[...] = jnp.zeros(l_ref.shape, jnp.float32)
    acc_ref[...] = jnp.zeros(acc_ref.shape, jnp.float32)

    def step(kb, masked):
        start = pl.multiple_of(kb * KB, KB)
        k = k_ref[pl.ds(start, KB), :]
        v = v_ref[pl.ds(start, KB), :]
        for h in range(heads):
            rows = slice(h * QB, (h + 1) * QB)
            s = lax.dot_general(q_of(h), k, (((1,), (1,)), ((), ())), preferred_element_type=jnp.float32)
            if masked:
                qp = pos0 + lax.broadcasted_iota(jnp.int32, (QB, KB), 0)
                kp = start + lax.broadcasted_iota(jnp.int32, (QB, KB), 1)
                s = jnp.where(kp <= qp, s, -jnp.inf)
            m_old = m_ref[rows, :]
            m_new = jnp.maximum(m_old, jnp.max(s, axis=1, keepdims=True))
            alpha = jnp.exp2((m_old - m_new) * c)
            p = jnp.exp2((s - jnp.concatenate([m_new] * (KB // 128), axis=1)) * c)
            lp = p[:, :128]
            for j in range(1, KB // 128):
                lp = lp + p[:, j * 128:(j + 1) * 128]
            m_ref[rows, :] = m_new
            l_ref[rows, :] = l_ref[rows, :] * alpha + lp
            acc_ref[rows, :] = acc_ref[rows, :] * alpha + jnp.dot(p.astype(jnp.bfloat16), v, preferred_element_type=jnp.float32)

    last = pos0 // KB

    def body(kb, carry):
        step(kb, False)
        return carry

    lax.fori_loop(0, last, body, 0)
    step(last, True)


def attn_kernel(cp_size, tp_size, heads, hd, q_ref, k_ref, v_ref, wo_ref, o_ref, m_ref, l_ref, acc_ref, ob_ref):
    b = pl.program_id(0)
    r = lax.axis_index('cp')
    t_src = b // 2
    half = b % 2
    seg = r + half * (2 * cp_size - 1 - 2 * r)
    pos0 = (seg * tp_size + t_src) * QB
    attend_block(lambda h: q_ref[:, h * hd:(h + 1) * hd], k_ref, v_ref, m_ref, l_ref, acc_ref, pos0, heads, hd)
    for h in range(heads):
        rows = slice(h * QB, (h + 1) * QB)
        den = jnp.sum(l_ref[rows, :], axis=1, keepdims=True)
        ob_ref[:, h * hd:(h + 1) * hd] = (acc_ref[rows, :] / den).astype(jnp.bfloat16)
    o_ref[...] = jnp.dot(ob_ref[...], wo_ref[...], preferred_element_type=jnp.float32)


def solution(mesh):
    cp_size = mesh.shape['cp']
    tp_size = mesh.shape['tp']
    num_devs = cp_size * tp_size
    row_spec = P(('data', 'cp', 'tp'), None)
    head_spec = P(None, 'tp', None)
    wo_spec = P('tp', None, None)
    expert_spec = P(('cp', 'tp'), None, None)

    def attention(queries, keys, vals, w_o, heads, hd):
        rows, width = queries.shape[0], w_o.shape[1]
        seq = keys.shape[0]
        full = lambda shape: pl.BlockSpec(shape, lambda b: (0, 0))
        return pl.pallas_call(
            functools.partial(attn_kernel, cp_size, tp_size, heads, hd),
            grid=(rows // QB,),
            in_specs=[pl.BlockSpec((QB, heads * hd), lambda b: (b, 0)), full((seq, hd)), full((seq, hd)), full((heads * hd, width))],
            out_specs=pl.BlockSpec((QB, width), lambda b: (b, 0)),
            out_shape=jax.ShapeDtypeStruct((rows, width), jnp.float32),
            scratch_shapes=[pltpu.VMEM((heads * QB, 128), jnp.float32), pltpu.VMEM((heads * QB, 128), jnp.float32), pltpu.VMEM((heads * QB, hd), jnp.float32), pltpu.VMEM((QB, heads * hd), jnp.bfloat16)],
            name='attn',
        )(queries, keys, vals, w_o)

    def device_fn(x_blk, w_q, w_k, w_v, w_o, idx_blk, gate_blk, w_gate, w_up, w_down):
        tok_dev, width = x_blk.shape
        heads, head_dim = w_q.shape[1], w_k.shape[2]
        exp_local = w_gate.shape[0]
        num_exp = exp_local * num_devs
        capacity = 4 * tok_dev // num_exp

        x_rows = lax.all_gather(x_blk, 'tp', axis=0, tiled=True)
        mm = lambda a, w: jnp.dot(a, w.reshape(width, -1), preferred_element_type=jnp.float32).astype(jnp.bfloat16)
        queries = mm(x_rows, w_q)
        kv_loc = jnp.stack([mm(x_rows, w_k), mm(x_rows, w_v)])
        kv_all = lax.all_gather(kv_loc, 'cp', axis=0)
        kv_all = kv_all.reshape(cp_size, 2, tp_size, 2, QB, head_dim)
        order = [kv_all[s, :, :, 0] for s in range(cp_size)] + [kv_all[cp_size - 1 - s, :, :, 1] for s in range(cp_size)]
        kv_pos = jnp.stack(order, axis=1).reshape(2, -1, head_dim)
        part_sum = attention(queries, kv_pos[0], kv_pos[1], w_o.reshape(heads * head_dim, width), heads, head_dim)
        attn_out = lax.psum_scatter(part_sum, 'tp', scatter_dimension=0, tiled=True)
        hidden = (x_blk.astype(jnp.float32) + attn_out).astype(jnp.bfloat16)

        flat_ids = idx_blk.reshape(-1)
        onehot = (flat_ids[:, None] == jnp.arange(num_exp)[None, :]).astype(jnp.int32)
        slot_pos = jnp.sum(jnp.cumsum(onehot, axis=0) * onehot, axis=1) - 1
        slot_ids = (flat_ids * capacity + slot_pos).reshape(tok_dev, 2)
        select = (slot_ids[:, :, None] == jnp.arange(num_exp * capacity)[None, None, :]).astype(jnp.bfloat16)
        send_buf = jnp.einsum('tkn,tm->nm', select, hidden, preferred_element_type=jnp.float32).astype(jnp.bfloat16)
        recv_buf = lax.all_to_all(send_buf, ('cp', 'tp'), 0, 0, tiled=True)
        tok_in = recv_buf.reshape(num_devs, exp_local, capacity, -1)
        gate_pre = jnp.einsum('secm,emf->secf', tok_in, w_gate, preferred_element_type=jnp.float32)
        up_pre = jnp.einsum('secm,emf->secf', tok_in, w_up, preferred_element_type=jnp.float32)
        hid_act = (jax.nn.silu(gate_pre) * up_pre).astype(jnp.bfloat16)
        exp_out = jnp.einsum('secf,efm->secm', hid_act, w_down, preferred_element_type=jnp.float32).astype(jnp.bfloat16)
        back_buf = lax.all_to_all(exp_out.reshape(num_devs * exp_local * capacity, -1), ('cp', 'tp'), 0, 0, tiled=True)
        picked = jnp.einsum('tkn,nm->tkm', select, back_buf, preferred_element_type=jnp.float32)
        moe_out = jnp.sum(gate_blk[:, :, None] * picked, axis=1)
        return (hidden.astype(jnp.float32) + moe_out).astype(jnp.bfloat16)

    return jax.shard_map(device_fn, mesh=mesh, in_specs=(row_spec, head_spec, head_spec, head_spec, wo_spec, row_spec, row_spec, expert_spec, expert_spec, expert_spec), out_specs=row_spec, check_vma=False)
```

```python
import functools
import jax
import jax.numpy as jnp
from jax import lax
from jax.experimental import pallas as pl
from jax.experimental.pallas import tpu as pltpu
from jax.sharding import PartitionSpec as P

QB = 256
KB = 512
LOG2E = 1.4426950408889634
VLIM = 60 * 1024 * 1024
MESH = pl.DeviceIdType.MESH


def attend_block(q_of, k_ref, v_ref, m_ref, l_ref, acc_ref, pos0, heads, hd):
    c = (hd ** -0.5) * LOG2E
    m_ref[...] = jnp.full(m_ref.shape, -jnp.inf, jnp.float32)
    l_ref[...] = jnp.zeros(l_ref.shape, jnp.float32)
    acc_ref[...] = jnp.zeros(acc_ref.shape, jnp.float32)

    def step(kb, masked):
        start = pl.multiple_of(kb * KB, KB)
        k = k_ref[pl.ds(start, KB), :]
        v = v_ref[pl.ds(start, KB), :]
        score = lambda h: lax.dot_general(q_of(h), k, (((1,), (1,)), ((), ())), preferred_element_type=jnp.float32)
        if masked:
            qp = pos0 + lax.broadcasted_iota(jnp.int32, (QB, KB), 0)
            kp = start + lax.broadcasted_iota(jnp.int32, (QB, KB), 1)
            keep = kp <= qp
        s_next = score(0)
        for h in range(heads):
            rows = slice(h * QB, (h + 1) * QB)
            s = s_next
            if h + 1 < heads:
                s_next = score(h + 1)
            if masked:
                s = jnp.where(keep, s, -jnp.inf)
            m_old = m_ref[rows, :]
            m_new = jnp.maximum(m_old, jnp.max(s, axis=1, keepdims=True))
            alpha = jnp.exp2((m_old - m_new) * c)
            p = jnp.exp2((s - jnp.concatenate([m_new] * (KB // 128), axis=1)) * c)
            lp = p[:, :128]
            for j in range(1, KB // 128):
                lp = lp + p[:, j * 128:(j + 1) * 128]
            m_ref[rows, :] = m_new
            l_ref[rows, :] = l_ref[rows, :] * alpha + lp
            acc_ref[rows, :] = acc_ref[rows, :] * alpha + jnp.dot(p.astype(jnp.bfloat16), v, preferred_element_type=jnp.float32)

    last = pos0 // KB

    def body(kb, carry):
        step(kb, False)
        return carry

    lax.fori_loop(0, last, body, 0)
    step(last, True)


def attn_kernel(cp_size, tp_size, heads, hd, q_ref, k_ref, v_ref, wo_ref, o_ref, m_ref, l_ref, acc_ref, ob_ref):
    b = pl.program_id(0)
    r = lax.axis_index('cp')
    t_src = b // 2
    half = b % 2
    seg = r + half * (2 * cp_size - 1 - 2 * r)
    pos0 = (seg * tp_size + t_src) * QB
    attend_block(lambda h: q_ref[:, h * hd:(h + 1) * hd], k_ref, v_ref, m_ref, l_ref, acc_ref, pos0, heads, hd)
    for h in range(heads):
        rows = slice(h * QB, (h + 1) * QB)
        den = jnp.sum(l_ref[rows, :], axis=1, keepdims=True)
        ob_ref[:, h * hd:(h + 1) * hd] = (acc_ref[rows, :] / den).astype(jnp.bfloat16)
    o_ref[...] = jnp.dot(ob_ref[...], wo_ref[...], preferred_element_type=jnp.float32)


def moe_kernel(num_devs, tp_size, exp_local, cap, h_ref, slot_ref, idx_ref, gate_ref, wg_ref, wu_ref, wd_ref, y_ref, hbuf, tok, wgb, wub, wdb, zrecv, yacc, hsem, wsem, send_sem, recv_sem):
    rows, width = y_ref.shape
    local_slots = exp_local * cap
    me = lax.axis_index('cp') * tp_size + lax.axis_index('tp')
    groups = recv_sem.shape[0]
    per_group = exp_local // groups

    barrier = pltpu.get_barrier_semaphore()
    for j in range(1, num_devs):
        other = lax.rem(me + j, num_devs)
        pl.semaphore_signal(barrier, inc=1, device_id=(0, other // tp_size, lax.rem(other, tp_size)), device_id_type=MESH)
    pl.semaphore_wait(barrier, num_devs - 1)

    def weight_copies(e, slot):
        return [pltpu.make_async_copy(src.at[e], dst.at[slot], wsem.at[i, slot]) for i, (src, dst) in enumerate(((wg_ref, wgb), (wu_ref, wub), (wd_ref, wdb)))]

    def h_copy(s, slot):
        return pltpu.make_async_copy(h_ref.at[pl.ds(pl.multiple_of(s * rows, rows), rows)], hbuf.at[slot], hsem.at[slot])

    h_copy(0, 0).start()
    for e in range(2):
        for copy in weight_copies(e, e):
            copy.start()

    def pick(s, carry):
        slot = lax.rem(s, 2)
        h_copy(s, slot).wait()

        @pl.when(s + 1 < num_devs)
        def _():
            h_copy(s + 1, 1 - slot).start()

        ids = slot_ref[s] - me * local_slots
        want = lax.broadcasted_iota(jnp.int32, (local_slots, rows), 0)
        sel = jnp.logical_or(ids[0:1, :] == want, ids[1:2, :] == want)
        sel = jnp.where(sel, 1.0, 0.0).astype(jnp.bfloat16)
        at = pl.multiple_of(s * cap, cap)
        for c0 in range(0, width, 512):
            part = jnp.dot(sel, hbuf[slot, :, c0:c0 + 512], preferred_element_type=jnp.float32).astype(jnp.bfloat16)
            tok[:, pl.ds(at, cap), c0:c0 + 512] = part.reshape(exp_local, cap, 512)

        @pl.when(s == me)
        def _():
            yacc[...] = hbuf[slot].astype(jnp.float32)

        return carry

    lax.fori_loop(0, num_devs, pick, 0)

    def expert(e, carry):
        slot = lax.rem(e, 2)
        for copy in weight_copies(e, slot):
            copy.wait()
        x = tok[e]
        gate = jnp.dot(x, wgb[slot], preferred_element_type=jnp.float32)
        up = jnp.dot(x, wub[slot], preferred_element_type=jnp.float32)
        act = (jax.nn.silu(gate) * up).astype(jnp.bfloat16)
        tok[e] = jnp.dot(act, wdb[slot], preferred_element_type=jnp.float32).astype(jnp.bfloat16)
        group = e // per_group
        for j in range(1, num_devs):
            other = lax.rem(me + j, num_devs)
            pltpu.make_async_remote_copy(
                src_ref=tok.at[e, pl.ds(pl.multiple_of(other * cap, cap), cap)],
                dst_ref=zrecv.at[e, pl.ds(pl.multiple_of(me * cap, cap), cap)],
                send_sem=send_sem,
                recv_sem=recv_sem.at[group],
                device_id=(0, other // tp_size, lax.rem(other, tp_size)),
                device_id_type=MESH,
            ).start()
        at = pl.ds(pl.multiple_of(me * cap, cap), cap)
        zrecv[e, at, :] = tok[e, at, :]

        @pl.when(e + 2 < exp_local)
        def _():
            for copy in weight_copies(e + 2, slot):
                copy.start()

        return carry

    lax.fori_loop(0, exp_local, expert, 0)

    span = per_group * num_devs * cap
    back = per_group * (num_devs - 1) * cap

    def combine(g, carry):
        whole = zrecv.at[pl.ds(0, per_group), pl.ds(0, (num_devs - 1) * cap)]
        pltpu.make_async_copy(whole, whole, recv_sem.at[g]).wait()
        want = lax.broadcasted_iota(jnp.int32, (rows, span), 1) + g * span
        sel0 = jnp.where(idx_ref[:, 0:1] == want, 1.0, 0.0).astype(jnp.bfloat16)
        sel1 = jnp.where(idx_ref[:, 1:2] == want, 1.0, 0.0).astype(jnp.bfloat16)
        first = pl.multiple_of(g * per_group, per_group)
        for c0 in range(0, width, 512):
            z = zrecv[pl.ds(first, per_group), :, c0:c0 + 512].reshape(span, 512)
            z0 = jnp.dot(sel0, z, preferred_element_type=jnp.float32)
            z1 = jnp.dot(sel1, z, preferred_element_type=jnp.float32)
            yacc[:, c0:c0 + 512] += gate_ref[:, 0:1] * z0 + gate_ref[:, 1:2] * z1
        return carry

    lax.fori_loop(0, groups, combine, 0)
    y_ref[...] = yacc[...].astype(y_ref.dtype)
    sent = tok.at[:, pl.ds(0, (num_devs - 1) * cap)]
    pltpu.make_async_copy(sent, sent, send_sem).wait()


def solution(mesh):
    cp_size = mesh.shape['cp']
    tp_size = mesh.shape['tp']
    num_devs = cp_size * tp_size
    row_spec = P(('data', 'cp', 'tp'), None)
    head_spec = P(None, 'tp', None)
    wo_spec = P('tp', None, None)
    expert_spec = P(('cp', 'tp'), None, None)

    def attention(queries, keys, vals, w_o, heads, hd):
        rows, width = queries.shape[0], w_o.shape[1]
        seq = keys.shape[0]
        full = lambda shape: pl.BlockSpec(shape, lambda b: (0, 0))
        return pl.pallas_call(
            functools.partial(attn_kernel, cp_size, tp_size, heads, hd),
            grid=(rows // QB,),
            in_specs=[pl.BlockSpec((QB, heads * hd), lambda b: (b, 0)), full((seq, hd)), full((seq, hd)), full((heads * hd, width))],
            out_specs=pl.BlockSpec((QB, width), lambda b: (b, 0)),
            out_shape=jax.ShapeDtypeStruct((rows, width), jnp.float32),
            scratch_shapes=[pltpu.VMEM((heads * QB, 128), jnp.float32), pltpu.VMEM((heads * QB, 128), jnp.float32), pltpu.VMEM((heads * QB, hd), jnp.float32), pltpu.VMEM((QB, heads * hd), jnp.bfloat16)],
            name='attn',
        )(queries, keys, vals, w_o)

    def experts(h_all, slots_all, back_idx, gates, w_gate, w_up, w_down, cap):
        rows, width = back_idx.shape[0], h_all.shape[1]
        exp_local, _, ff = w_gate.shape
        vmem = pl.BlockSpec(memory_space=pltpu.VMEM)
        hbm = pl.BlockSpec(memory_space=pl.ANY)
        bf16 = jnp.bfloat16
        dma = pltpu.SemaphoreType.DMA
        return pl.pallas_call(
            functools.partial(moe_kernel, num_devs, tp_size, exp_local, cap),
            in_specs=[hbm, vmem, vmem, vmem, hbm, hbm, hbm],
            out_specs=vmem,
            out_shape=jax.ShapeDtypeStruct((rows, width), bf16),
            scratch_shapes=[pltpu.VMEM((2, rows, width), bf16), pltpu.VMEM((exp_local, num_devs * cap, width), bf16), pltpu.VMEM((2, width, ff), bf16), pltpu.VMEM((2, width, ff), bf16), pltpu.VMEM((2, ff, width), bf16), pltpu.VMEM((exp_local, num_devs * cap, width), bf16), pltpu.VMEM((rows, width), jnp.float32), dma((2,)), dma((3, 2)), dma, dma((4,))],
            compiler_params=pltpu.CompilerParams(collective_id=2, has_side_effects=True, vmem_limit_bytes=VLIM),
            name='moe',
        )(h_all, slots_all, back_idx, gates, w_gate, w_up, w_down)

    def device_fn(x_blk, w_q, w_k, w_v, w_o, idx_blk, gate_blk, w_gate, w_up, w_down):
        tok_dev, width = x_blk.shape
        heads, head_dim = w_q.shape[1], w_k.shape[2]
        exp_local = w_gate.shape[0]
        num_exp = exp_local * num_devs
        capacity = 4 * tok_dev // num_exp

        x_rows = lax.all_gather(x_blk, 'tp', axis=0, tiled=True)
        mm = lambda a, w: jnp.dot(a, w.reshape(width, -1), preferred_element_type=jnp.float32).astype(jnp.bfloat16)
        queries = mm(x_rows, w_q)
        kv_loc = jnp.stack([mm(x_rows, w_k), mm(x_rows, w_v)])
        kv_all = lax.all_gather(kv_loc, 'cp', axis=0)
        kv_all = kv_all.reshape(cp_size, 2, tp_size, 2, QB, head_dim)
        order = [kv_all[s, :, :, 0] for s in range(cp_size)] + [kv_all[cp_size - 1 - s, :, :, 1] for s in range(cp_size)]
        kv_pos = jnp.stack(order, axis=1).reshape(2, -1, head_dim)
        part_sum = attention(queries, kv_pos[0], kv_pos[1], w_o.reshape(heads * head_dim, width), heads, head_dim)
        attn_out = lax.psum_scatter(part_sum, 'tp', scatter_dimension=0, tiled=True)
        hidden = (x_blk.astype(jnp.float32) + attn_out).astype(jnp.bfloat16)

        flat_ids = idx_blk.reshape(-1)
        onehot = (flat_ids[:, None] == jnp.arange(num_exp)[None, :]).astype(jnp.int32)
        slot_pos = jnp.sum(jnp.cumsum(onehot, axis=0) * onehot, axis=1) - 1
        slot_ids = (flat_ids * capacity + slot_pos).reshape(tok_dev, 2)
        slots_all = lax.all_gather(slot_ids.T, ('cp', 'tp'), axis=0)
        back_idx = (slot_ids // capacity % exp_local) * (num_devs * capacity) + slot_ids // (capacity * exp_local) * capacity + slot_ids % capacity
        h_all = lax.all_gather(hidden, ('cp', 'tp'), axis=0, tiled=True)
        return experts(h_all, slots_all, back_idx, gate_blk, w_gate, w_up, w_down, capacity)

    return jax.shard_map(device_fn, mesh=mesh, in_specs=(row_spec, head_spec, head_spec, head_spec, wo_spec, row_spec, row_spec, expert_spec, expert_spec, expert_spec), out_specs=row_spec, check_vma=False)
```

```python
import functools
import jax
import jax.numpy as jnp
from jax import lax
from jax.experimental import pallas as pl
from jax.experimental.pallas import tpu as pltpu
from jax.sharding import PartitionSpec as P

QB = 256
KB = 512
CH = 128
LOG2E = 1.4426950408889634
VLIM = 60 * 1024 * 1024
MESH = pl.DeviceIdType.MESH


def attend_block(q_of, kv_ref, m_ref, l_ref, acc_ref, pos0, heads, hd):
    c = (hd ** -0.5) * LOG2E
    m_ref[...] = jnp.full(m_ref.shape, -jnp.inf, jnp.float32)
    l_ref[...] = jnp.zeros(l_ref.shape, jnp.float32)
    acc_ref[...] = jnp.zeros(acc_ref.shape, jnp.float32)

    def step(kb, masked):
        start = pl.multiple_of(kb * KB, KB)
        k = kv_ref[pl.ds(start, KB), :hd]
        v = kv_ref[pl.ds(start, KB), hd:]
        score = lambda h: lax.dot_general(q_of(h), k, (((1,), (1,)), ((), ())), preferred_element_type=jnp.float32)
        if masked:
            qp = pos0 + lax.broadcasted_iota(jnp.int32, (QB, KB), 0)
            kp = start + lax.broadcasted_iota(jnp.int32, (QB, KB), 1)
            keep = kp <= qp
        s_next = score(0)
        for h in range(heads):
            rows = slice(h * QB, (h + 1) * QB)
            s = s_next
            if h + 1 < heads:
                s_next = score(h + 1)
            if masked:
                s = jnp.where(keep, s, -jnp.inf)
            m_old = m_ref[rows, :]
            m_new = jnp.maximum(m_old, jnp.max(s, axis=1, keepdims=True))
            alpha = jnp.exp2((m_old - m_new) * c)
            p = jnp.exp2((s - jnp.concatenate([m_new] * (KB // 128), axis=1)) * c)
            lp = p[:, :128]
            for j in range(1, KB // 128):
                lp = lp + p[:, j * 128:(j + 1) * 128]
            m_ref[rows, :] = m_new
            l_ref[rows, :] = l_ref[rows, :] * alpha + lp
            acc_ref[rows, :] = acc_ref[rows, :] * alpha + jnp.dot(p.astype(jnp.bfloat16), v, preferred_element_type=jnp.float32)

    last = pos0 // KB

    def body(kb, carry):
        step(kb, False)
        return carry

    lax.fori_loop(0, last, body, 0)
    step(last, True)


def rdma(src, dst, send_sem, recv_sem, cp, tp):
    return pltpu.make_async_remote_copy(src_ref=src, dst_ref=dst, send_sem=send_sem, recv_sem=recv_sem, device_id=(0, cp, tp), device_id_type=MESH)


def await_bytes(ref, sem):
    pltpu.make_async_copy(ref, ref, sem).wait()


def greet(others):
    barrier = pltpu.get_barrier_semaphore()
    for cp, tp in others:
        pl.semaphore_signal(barrier, inc=1, device_id=(0, cp, tp), device_id_type=MESH)
    pl.semaphore_wait(barrier, len(others))


def qkv_kernel(cp_size, tp_size, x_ref, slot_ref, wq_ref, wk_ref, wv_ref, q_ref, kv_ref, slots_ref, x_all, wq, wkv, wsem, slot_send, slot_recv, own_send, x_recv, near_recv, fwd_send, fwd_recv, kv_send, kv_recv, slot_sem):
    r, t = lax.axis_index('cp'), lax.axis_index('tp')
    num_devs = cp_size * tp_size
    me = r * tp_size + t
    near = t + 1 - 2 * lax.rem(t, 2)
    far = lax.rem(t + 2, tp_size)
    far_near = lax.rem(near + 2, tp_size)
    peer = 1 - r
    rows = x_ref.shape[0]
    half_rows = rows // 2
    hd = wk_ref.shape[1]
    devs = [lax.rem(me + j, num_devs) for j in range(1, num_devs)]

    weights = [pltpu.make_async_copy(wk_ref, wkv.at[:, pl.ds(0, hd)], wsem.at[0]), pltpu.make_async_copy(wv_ref, wkv.at[:, pl.ds(hd, hd)], wsem.at[1]), pltpu.make_async_copy(wq_ref, wq, wsem.at[2])]
    for copy in weights:
        copy.start()
    greet([(d // tp_size, lax.rem(d, tp_size)) for d in devs])
    chunks = rows // CH
    for j in range(chunks):
        at = pl.ds(j * CH, CH)
        rdma(x_ref.at[at], x_all.at[t, at], own_send, x_recv.at[j], r, far).start()
    rdma(x_ref, x_all.at[t], own_send, near_recv, r, near).start()
    for d in devs:
        rdma(slot_ref, slots_ref.at[me], slot_send, slot_recv, d // tp_size, lax.rem(d, tp_size)).start()
    mine = pltpu.make_async_copy(slot_ref, slots_ref.at[me], slot_sem)
    mine.start()
    for copy in weights:
        copy.wait()

    def project(x, tp_src, row0, count):
        half = row0 // half_rows
        seg = r + half * (2 * cp_size - 1 - 2 * r)
        pos = pl.multiple_of((seg * tp_size + tp_src) * half_rows + row0 % half_rows, CH)
        kv_ref[pl.ds(pos, count), :] = jnp.dot(x, wkv[...], preferred_element_type=jnp.float32).astype(jnp.bfloat16)
        sent = kv_ref.at[pl.ds(pos, count)]
        rdma(sent, sent, kv_send, kv_recv, peer, t).start()
        at = pl.ds(pl.multiple_of(tp_src * rows + row0, CH), count)
        q_ref[at, :] = jnp.dot(x, wq[...], preferred_element_type=jnp.float32).astype(jnp.bfloat16)

    for half in range(2):
        project(x_ref[half * half_rows:(half + 1) * half_rows, :], t, half * half_rows, half_rows)
    await_bytes(x_all.at[near], near_recv)
    for half in range(2):
        project(x_all[near, half * half_rows:(half + 1) * half_rows, :], near, half * half_rows, half_rows)
    for j in range(chunks):
        at = pl.ds(j * CH, CH)
        await_bytes(x_all.at[far, at], x_recv.at[j])
        rdma(x_all.at[far, at], x_all.at[far, at], fwd_send, fwd_recv.at[j], r, near).start()
        project(x_all[far, j * CH:(j + 1) * CH, :], far, j * CH, CH)
        await_bytes(x_all.at[far_near, at], fwd_recv.at[j])
        project(x_all[far_near, j * CH:(j + 1) * CH, :], far_near, j * CH, CH)

    mine.wait()
    await_bytes(slots_ref.at[pl.ds(0, num_devs - 1)], slot_recv)
    await_bytes(slots_ref.at[pl.ds(0, num_devs - 1)], slot_send)
    await_bytes(x_all.at[pl.ds(0, 2)], own_send)
    await_bytes(x_all.at[0], fwd_send)
    half_kv = kv_ref.at[pl.ds(0, tp_size * rows)]
    await_bytes(half_kv, kv_recv)
    await_bytes(half_kv, kv_send)


def block_kernel(cp_size, tp_size, heads, hd, q_ref, kv_ref, wo_ref, x_ref, h_ref, m_ref, l_ref, acc_ref, ob_ref, part, from_near, from_far, hbuf, near_send, near_recv, far_send, far_recv, h_send, h_near, h_far, h_peer, h_diag, h_own):
    r, t = lax.axis_index('cp'), lax.axis_index('tp')
    me = r * tp_size + t
    near = t + 1 - 2 * lax.rem(t, 2)
    far = lax.rem(t + 2, tp_size)
    peer = 1 - r
    rows, width = x_ref.shape
    greet([(r, near), (r, far), (peer, t)])

    def block(i, carry):
        local = i // 4
        mine = lax.rem(i, 2)
        half = lax.rem(i // 2, 2)
        t_dst = lax.rem(mine * t + (1 - mine) * near + 2 * (1 - local), tp_size)
        seg = r + half * (2 * cp_size - 1 - 2 * r)
        pos0 = (seg * tp_size + t_dst) * QB
        row0 = pl.multiple_of(t_dst * rows + half * QB, QB)
        attend_block(lambda h: q_ref[pl.ds(row0, QB), h * hd:(h + 1) * hd], kv_ref, m_ref, l_ref, acc_ref, pos0, heads, hd)
        for h in range(heads):
            at = slice(h * QB, (h + 1) * QB)
            den = jnp.sum(l_ref[at, :], axis=1, keepdims=True)
            ob_ref[:, h * hd:(h + 1) * hd] = (acc_ref[at, :] / den).astype(jnp.bfloat16)
        part[i] = jnp.dot(ob_ref[...], wo_ref[...], preferred_element_type=jnp.float32)

        @pl.when(mine == 0)
        def _():
            rdma(part.at[i], from_near.at[i // 2], near_send, near_recv.at[i // 2], r, near).start()

        @pl.when(jnp.logical_and(mine == 1, local == 0))
        def _():
            await_bytes(from_near.at[half], near_recv.at[half])
            part[i] += from_near[half]
            for c in range(QB // CH):
                at = pl.ds(c * CH, CH)
                rdma(part.at[i, at], from_far.at[half, at], far_send, far_recv.at[half, c], r, far).start()

        return carry

    lax.fori_loop(0, 8, block, 0)

    def h_rows(cp, tp, j):
        return h_ref.at[pl.ds(pl.multiple_of((cp * tp_size + tp) * rows + j * CH, CH), CH)]

    per_half = QB // CH
    chunks = rows // CH
    for j in range(chunks):
        half, c = j // per_half, j % per_half
        at = slice(c * CH, (c + 1) * CH)
        if c == 0:
            await_bytes(from_near.at[2 + half], near_recv.at[2 + half])
        await_bytes(from_far.at[half, pl.ds(c * CH, CH)], far_recv.at[half, c])
        total = part[5 + 2 * half, at, :] + from_near[2 + half, at, :] + from_far[half, at, :]
        hbuf[j] = (x_ref[j * CH:(j + 1) * CH, :].astype(jnp.float32) + total).astype(jnp.bfloat16)
        mine = h_rows(r, t, j)
        rdma(hbuf.at[j], mine, h_send, h_far.at[j], r, far).start()
        rdma(hbuf.at[j], mine, h_send, h_peer.at[j], peer, t).start()
        rdma(hbuf.at[j], mine, h_send, h_near, r, near).start()
        pltpu.make_async_copy(hbuf.at[j], mine, h_own).start()
        got = h_rows(peer, t, j)
        await_bytes(got, h_peer.at[j])
        rdma(got, got, h_send, h_near, r, near).start()

    def diag(j):
        got = h_rows(peer, far, j)
        await_bytes(got, h_diag.at[j])
        rdma(got, got, h_send, h_near, r, near).start()

    for j in range(chunks):
        got = h_rows(r, far, j)
        await_bytes(got, h_far.at[j])
        rdma(got, got, h_send, h_diag.at[j], peer, t).start()
        rdma(got, got, h_send, h_near, r, near).start()
        if j > 0:
            diag(j - 1)
    diag(chunks - 1)

    await_bytes(h_ref.at[pl.ds(0, 4 * rows)], h_near)
    await_bytes(h_ref.at[pl.ds(0, 7 * rows)], h_send)
    await_bytes(h_ref.at[pl.ds(0, rows)], h_own)
    await_bytes(part.at[pl.ds(0, 4)], near_send)
    await_bytes(part.at[pl.ds(0, 2)], far_send)


def moe_kernel(num_devs, tp_size, exp_local, cap, h_ref, slot_ref, idx_ref, gate_ref, wg_ref, wu_ref, wd_ref, y_ref, hbuf, tok, wgb, wub, wdb, zrecv, yacc, hsem, wsem, send_sem, recv_sem):
    rows, width = y_ref.shape
    local_slots = exp_local * cap
    me = lax.axis_index('cp') * tp_size + lax.axis_index('tp')
    groups = recv_sem.shape[0]
    per_group = exp_local // groups

    barrier = pltpu.get_barrier_semaphore()
    for j in range(1, num_devs):
        other = lax.rem(me + j, num_devs)
        pl.semaphore_signal(barrier, inc=1, device_id=(0, other // tp_size, lax.rem(other, tp_size)), device_id_type=MESH)
    pl.semaphore_wait(barrier, num_devs - 1)

    def weight_copies(e, slot):
        return [pltpu.make_async_copy(src.at[e], dst.at[slot], wsem.at[i, slot]) for i, (src, dst) in enumerate(((wg_ref, wgb), (wu_ref, wub), (wd_ref, wdb)))]

    def h_copy(s, slot):
        return pltpu.make_async_copy(h_ref.at[pl.ds(pl.multiple_of(s * rows, rows), rows)], hbuf.at[slot], hsem.at[slot])

    h_copy(0, 0).start()
    for e in range(2):
        for copy in weight_copies(e, e):
            copy.start()

    def pick(s, carry):
        slot = lax.rem(s, 2)
        h_copy(s, slot).wait()

        @pl.when(s + 1 < num_devs)
        def _():
            h_copy(s + 1, 1 - slot).start()

        ids = slot_ref[s] - me * local_slots
        want = lax.broadcasted_iota(jnp.int32, (local_slots, rows), 0)
        sel = jnp.logical_or(ids[0:1, :] == want, ids[1:2, :] == want)
        sel = jnp.where(sel, 1.0, 0.0).astype(jnp.bfloat16)
        at = pl.multiple_of(s * cap, cap)
        for c0 in range(0, width, 512):
            part = jnp.dot(sel, hbuf[slot, :, c0:c0 + 512], preferred_element_type=jnp.float32).astype(jnp.bfloat16)
            tok[:, pl.ds(at, cap), c0:c0 + 512] = part.reshape(exp_local, cap, 512)

        @pl.when(s == me)
        def _():
            yacc[...] = hbuf[slot].astype(jnp.float32)

        return carry

    lax.fori_loop(0, num_devs, pick, 0)

    def expert(e, carry):
        slot = lax.rem(e, 2)
        for copy in weight_copies(e, slot):
            copy.wait()
        x = tok[e]
        gate = jnp.dot(x, wgb[slot], preferred_element_type=jnp.float32)
        up = jnp.dot(x, wub[slot], preferred_element_type=jnp.float32)
        act = (jax.nn.silu(gate) * up).astype(jnp.bfloat16)
        tok[e] = jnp.dot(act, wdb[slot], preferred_element_type=jnp.float32).astype(jnp.bfloat16)
        group = e // per_group
        for j in range(1, num_devs):
            other = lax.rem(me + j, num_devs)
            pltpu.make_async_remote_copy(
                src_ref=tok.at[e, pl.ds(pl.multiple_of(other * cap, cap), cap)],
                dst_ref=zrecv.at[e, pl.ds(pl.multiple_of(me * cap, cap), cap)],
                send_sem=send_sem,
                recv_sem=recv_sem.at[group],
                device_id=(0, other // tp_size, lax.rem(other, tp_size)),
                device_id_type=MESH,
            ).start()
        at = pl.ds(pl.multiple_of(me * cap, cap), cap)
        zrecv[e, at, :] = tok[e, at, :]

        @pl.when(e + 2 < exp_local)
        def _():
            for copy in weight_copies(e + 2, slot):
                copy.start()

        return carry

    lax.fori_loop(0, exp_local, expert, 0)

    span = per_group * num_devs * cap
    back = per_group * (num_devs - 1) * cap

    def combine(g, carry):
        whole = zrecv.at[pl.ds(0, per_group), pl.ds(0, (num_devs - 1) * cap)]
        pltpu.make_async_copy(whole, whole, recv_sem.at[g]).wait()
        want = lax.broadcasted_iota(jnp.int32, (rows, span), 1) + g * span
        sel0 = jnp.where(idx_ref[:, 0:1] == want, 1.0, 0.0).astype(jnp.bfloat16)
        sel1 = jnp.where(idx_ref[:, 1:2] == want, 1.0, 0.0).astype(jnp.bfloat16)
        first = pl.multiple_of(g * per_group, per_group)
        for c0 in range(0, width, 512):
            z = zrecv[pl.ds(first, per_group), :, c0:c0 + 512].reshape(span, 512)
            z0 = jnp.dot(sel0, z, preferred_element_type=jnp.float32)
            z1 = jnp.dot(sel1, z, preferred_element_type=jnp.float32)
            yacc[:, c0:c0 + 512] += gate_ref[:, 0:1] * z0 + gate_ref[:, 1:2] * z1
        return carry

    lax.fori_loop(0, groups, combine, 0)
    y_ref[...] = yacc[...].astype(y_ref.dtype)
    sent = tok.at[:, pl.ds(0, (num_devs - 1) * cap)]
    pltpu.make_async_copy(sent, sent, send_sem).wait()


def solution(mesh):
    cp_size = mesh.shape['cp']
    tp_size = mesh.shape['tp']
    num_devs = cp_size * tp_size
    row_spec = P(('data', 'cp', 'tp'), None)
    head_spec = P(None, 'tp', None)
    wo_spec = P('tp', None, None)
    expert_spec = P(('cp', 'tp'), None, None)

    vmem = pl.BlockSpec(memory_space=pltpu.VMEM)
    hbm = pl.BlockSpec(memory_space=pl.ANY)
    dma = pltpu.SemaphoreType.DMA
    bf16, f32 = jnp.bfloat16, jnp.float32

    def params(number):
        return pltpu.CompilerParams(collective_id=number, has_side_effects=True, vmem_limit_bytes=VLIM)

    def project(x_blk, slot_ids, w_q, w_k, w_v):
        rows, width = x_blk.shape
        q_width, kv_width = w_q.shape[1], w_k.shape[1]
        group = rows * tp_size
        return pl.pallas_call(
            functools.partial(qkv_kernel, cp_size, tp_size),
            in_specs=[vmem, vmem, hbm, hbm, hbm],
            out_specs=[vmem, vmem, vmem],
            out_shape=[jax.ShapeDtypeStruct((group, q_width), bf16), jax.ShapeDtypeStruct((group * cp_size, 2 * kv_width), bf16), jax.ShapeDtypeStruct((num_devs,) + slot_ids.shape, jnp.int32)],
            scratch_shapes=[pltpu.VMEM((tp_size, rows, width), bf16), pltpu.VMEM((width, q_width), bf16), pltpu.VMEM((width, 2 * kv_width), bf16), dma((3,)), dma, dma, dma, dma((rows // CH,)), dma, dma, dma((rows // CH,)), dma, dma, dma],
            compiler_params=params(0),
            name='qkv',
        )(x_blk, slot_ids, w_q, w_k, w_v)

    def attention(q, kv, w_o, x_blk, heads, hd):
        rows, width = x_blk.shape
        v32 = lambda *shape: pltpu.VMEM(shape, f32)
        chunks = rows // CH
        return pl.pallas_call(
            functools.partial(block_kernel, cp_size, tp_size, heads, hd),
            in_specs=[vmem, vmem, vmem, vmem],
            out_specs=hbm,
            out_shape=jax.ShapeDtypeStruct((rows * num_devs, width), bf16),
            scratch_shapes=[v32(heads * QB, 128), v32(heads * QB, 128), v32(heads * QB, hd), pltpu.VMEM((QB, heads * hd), bf16), v32(8, QB, width), v32(4, QB, width), v32(2, QB, width), pltpu.VMEM((chunks, CH, width), bf16), dma, dma((4,)), dma, dma((2, QB // CH)), dma, dma, dma((chunks,)), dma((chunks,)), dma((chunks,)), dma],
            compiler_params=params(1),
            name='attn',
        )(q, kv, w_o, x_blk)

    def experts(h_all, slots_all, back_idx, gates, w_gate, w_up, w_down, cap):
        rows, width = back_idx.shape[0], h_all.shape[1]
        exp_local, _, ff = w_gate.shape
        return pl.pallas_call(
            functools.partial(moe_kernel, num_devs, tp_size, exp_local, cap),
            in_specs=[hbm, vmem, vmem, vmem, hbm, hbm, hbm],
            out_specs=vmem,
            out_shape=jax.ShapeDtypeStruct((rows, width), bf16),
            scratch_shapes=[pltpu.VMEM((2, rows, width), bf16), pltpu.VMEM((exp_local, num_devs * cap, width), bf16), pltpu.VMEM((2, width, ff), bf16), pltpu.VMEM((2, width, ff), bf16), pltpu.VMEM((2, ff, width), bf16), pltpu.VMEM((exp_local, num_devs * cap, width), bf16), pltpu.VMEM((rows, width), jnp.float32), dma((2,)), dma((3, 2)), dma, dma((4,))],
            compiler_params=params(2),
            name='moe',
        )(h_all, slots_all, back_idx, gates, w_gate, w_up, w_down)

    def device_fn(x_blk, w_q, w_k, w_v, w_o, idx_blk, gate_blk, w_gate, w_up, w_down):
        tok_dev, width = x_blk.shape
        heads, head_dim = w_q.shape[1], w_k.shape[2]
        exp_local = w_gate.shape[0]
        num_exp = exp_local * num_devs
        capacity = 4 * tok_dev // num_exp

        flat_ids = idx_blk.reshape(-1)
        onehot = (flat_ids[:, None] == jnp.arange(num_exp)[None, :]).astype(jnp.int32)
        slot_pos = jnp.sum(jnp.cumsum(onehot, axis=0) * onehot, axis=1) - 1
        slot_ids = (flat_ids * capacity + slot_pos).reshape(tok_dev, 2)
        back_idx = (slot_ids // capacity % exp_local) * (num_devs * capacity) + slot_ids // (capacity * exp_local) * capacity + slot_ids % capacity
        flat = lambda w: w.reshape(width, -1)
        q, kv, slots_all = project(x_blk, slot_ids.T, flat(w_q), flat(w_k), flat(w_v))
        h_all = attention(q, kv, w_o.reshape(heads * head_dim, width), x_blk, heads, head_dim)
        return experts(h_all, slots_all, back_idx, gate_blk, w_gate, w_up, w_down, capacity)

    return jax.shard_map(device_fn, mesh=mesh, in_specs=(row_spec, head_spec, head_spec, head_spec, wo_spec, row_spec, row_spec, expert_spec, expert_spec, expert_spec), out_specs=row_spec, check_vma=False)
```

```python
import functools
import jax
import jax.numpy as jnp
from jax import lax
from jax.experimental import pallas as pl
from jax.experimental.pallas import tpu as pltpu
from jax.sharding import PartitionSpec as P

QB = 256
KB = 512
CH = 128
HC = 64
LOG2E = 1.4426950408889634
VLIM = 60 * 1024 * 1024
MESH = pl.DeviceIdType.MESH


def attend_block(q_of, kv_ref, m_ref, l_ref, acc_ref, pos0, heads, hd):
    c = (hd ** -0.5) * LOG2E
    m_ref[...] = jnp.full(m_ref.shape, -jnp.inf, jnp.float32)
    l_ref[...] = jnp.zeros(l_ref.shape, jnp.float32)
    acc_ref[...] = jnp.zeros(acc_ref.shape, jnp.float32)

    def step(kb, masked):
        start = pl.multiple_of(kb * KB, KB)
        k = kv_ref[pl.ds(start, KB), :hd]
        v = kv_ref[pl.ds(start, KB), hd:]
        score = lambda h: lax.dot_general(q_of(h), k, (((1,), (1,)), ((), ())), preferred_element_type=jnp.float32)
        if masked:
            qp = pos0 + lax.broadcasted_iota(jnp.int32, (QB, KB), 0)
            kp = start + lax.broadcasted_iota(jnp.int32, (QB, KB), 1)
            keep = kp <= qp
        s_next = score(0)
        for h in range(heads):
            rows = slice(h * QB, (h + 1) * QB)
            s = s_next
            if h + 1 < heads:
                s_next = score(h + 1)
            if masked:
                s = jnp.where(keep, s, -jnp.inf)
            m_old = m_ref[rows, :]
            m_new = jnp.maximum(m_old, jnp.max(s, axis=1, keepdims=True))
            alpha = jnp.exp2((m_old - m_new) * c)
            p = jnp.exp2((s - jnp.concatenate([m_new] * (KB // 128), axis=1)) * c)
            lp = p[:, :128]
            for j in range(1, KB // 128):
                lp = lp + p[:, j * 128:(j + 1) * 128]
            m_ref[rows, :] = m_new
            l_ref[rows, :] = l_ref[rows, :] * alpha + lp
            acc_ref[rows, :] = acc_ref[rows, :] * alpha + jnp.dot(p.astype(jnp.bfloat16), v, preferred_element_type=jnp.float32)

    last = pos0 // KB

    def body(kb, carry):
        step(kb, False)
        return carry

    lax.fori_loop(0, last, body, 0)
    step(last, True)


def rdma(src, dst, send_sem, recv_sem, cp, tp):
    return pltpu.make_async_remote_copy(src_ref=src, dst_ref=dst, send_sem=send_sem, recv_sem=recv_sem, device_id=(0, cp, tp), device_id_type=MESH)


def await_bytes(ref, sem):
    pltpu.make_async_copy(ref, ref, sem).wait()


def greet(others):
    barrier = pltpu.get_barrier_semaphore()
    for cp, tp in others:
        pl.semaphore_signal(barrier, inc=1, device_id=(0, cp, tp), device_id_type=MESH)
    pl.semaphore_wait(barrier, len(others))


def slot_rows(idx_ref, num_exp, cap):
    rows = idx_ref.shape[1]
    expert = lax.broadcasted_iota(jnp.int32, (num_exp, rows), 0)
    hot = [jnp.where(idx_ref[k:k + 1, :] == expert, 1.0, 0.0) for k in range(2)]
    earlier = lax.broadcasted_iota(jnp.int32, (rows, rows), 0) < lax.broadcasted_iota(jnp.int32, (rows, rows), 1)
    earlier = jnp.where(earlier, 1.0, 0.0).astype(jnp.bfloat16)
    count = jnp.dot((hot[0] + hot[1]).astype(jnp.bfloat16), earlier, preferred_element_type=jnp.float32)
    return [idx_ref[k:k + 1, :] * cap + jnp.sum(hot[k] * count, axis=0, keepdims=True).astype(jnp.int32) for k in range(2)]


def front_kernel(cp_size, tp_size, heads, hd, num_exp, cap, x_ref, idx_ref, wq_ref, wk_ref, wv_ref, wo_ref, h_ref, tok_ref, hbuf, own_slots,
                 x_all, wq, wkv, wo, q_ref, kv_ref, slots, m_ref, l_ref, acc_ref, ob_ref, part, from_near, from_far,
                 wsem, slot_send, slot_recv, x_send, x_near, x_far, x_fwd_send, x_fwd, kv_send, kv_recv,
                 near_send, near_recv, far_send, far_recv, h_send, h_near, h_far, h_peer, h_diag, load_sem, tok_sem):
    r, t = lax.axis_index('cp'), lax.axis_index('tp')
    num_devs = cp_size * tp_size
    me = r * tp_size + t
    near = t + 1 - 2 * lax.rem(t, 2)
    far = lax.rem(t + 2, tp_size)
    far_near = lax.rem(near + 2, tp_size)
    peer = 1 - r
    rows, width = x_ref.shape
    half_rows = rows // 2
    devs = [lax.rem(me + j, num_devs) for j in range(1, num_devs)]

    weights = [pltpu.make_async_copy(wk_ref, wkv.at[:, pl.ds(0, hd)], wsem.at[0]), pltpu.make_async_copy(wv_ref, wkv.at[:, pl.ds(hd, hd)], wsem.at[1]), pltpu.make_async_copy(wq_ref, wq, wsem.at[2]), pltpu.make_async_copy(wo_ref, wo, wsem.at[3])]
    for copy in weights:
        copy.start()
    greet([(d // tp_size, lax.rem(d, tp_size)) for d in devs])
    chunks = rows // CH
    for j in range(chunks):
        at = pl.ds(j * CH, CH)
        rdma(x_ref.at[at], x_all.at[0, at], x_send, x_far.at[j], r, far).start()
    rdma(x_ref, x_all.at[1], x_send, x_near, r, near).start()
    mine = slot_rows(idx_ref, num_exp, cap)
    own_slots[...] = jnp.concatenate(mine + [jnp.zeros((6, rows), jnp.int32)], axis=0)
    slots[me] = own_slots[...]
    for d in devs:
        rdma(own_slots, slots.at[me], slot_send, slot_recv, d // tp_size, lax.rem(d, tp_size)).start()
    for copy in weights[:3]:
        copy.wait()

    def project(x, tp_src, row0, count):
        half = row0 // half_rows
        seg = r + half * (2 * cp_size - 1 - 2 * r)
        pos = pl.multiple_of((seg * tp_size + tp_src) * half_rows + row0 % half_rows, CH)
        kv_ref[pl.ds(pos, count), :] = jnp.dot(x, wkv[...], preferred_element_type=jnp.float32).astype(jnp.bfloat16)
        sent = kv_ref.at[pl.ds(pos, count)]
        rdma(sent, sent, kv_send, kv_recv.at[half], peer, t).start()
        at = pl.ds(pl.multiple_of(tp_src * rows + row0, CH), count)
        q_ref[at, :] = jnp.dot(x, wq[...], preferred_element_type=jnp.float32).astype(jnp.bfloat16)

    def project_far(half):
        for j in range(half * (chunks // 2), (half + 1) * (chunks // 2)):
            at = pl.ds(j * CH, CH)
            await_bytes(x_all.at[0, at], x_far.at[j])
            rdma(x_all.at[0, at], x_all.at[2, at], x_fwd_send, x_fwd.at[j], r, near).start()
            project(x_all[0, j * CH:(j + 1) * CH, :], far, j * CH, CH)
            await_bytes(x_all.at[2, at], x_fwd.at[j])
            project(x_all[2, j * CH:(j + 1) * CH, :], far_near, j * CH, CH)
        await_bytes(kv_ref.at[pl.ds(0, tp_size * half_rows)], kv_recv.at[half])

    for half in range(2):
        project(x_ref[half * half_rows:(half + 1) * half_rows, :], t, half * half_rows, half_rows)
    await_bytes(x_all.at[1], x_near)
    for half in range(2):
        project(x_all[1, half * half_rows:(half + 1) * half_rows, :], near, half * half_rows, half_rows)
    project_far(0)
    weights[3].wait()

    def block(i, carry):
        local = i // 4
        mine = lax.rem(i, 2)
        half = lax.rem(i // 2, 2)
        slot = mine * (2 + 2 * local) + half

        @pl.when(i == 2)
        def _():
            project_far(1)

        @pl.when(jnp.logical_and(mine == 0, local == 1))
        def _():
            await_bytes(part.at[half], near_send.at[half])

        t_dst = lax.rem(mine * t + (1 - mine) * near + 2 * (1 - local), tp_size)
        seg = r + half * (2 * cp_size - 1 - 2 * r)
        pos0 = (seg * tp_size + t_dst) * QB
        row0 = pl.multiple_of(t_dst * rows + half * QB, QB)
        attend_block(lambda h: q_ref[pl.ds(row0, QB), h * hd:(h + 1) * hd], kv_ref, m_ref, l_ref, acc_ref, pos0, heads, hd)
        for h in range(heads):
            at = slice(h * QB, (h + 1) * QB)
            den = jnp.sum(l_ref[at, :], axis=1, keepdims=True)
            ob_ref[:, h * hd:(h + 1) * hd] = (acc_ref[at, :] / den).astype(jnp.bfloat16)
        part[slot] = jnp.dot(ob_ref[...], wo[...], preferred_element_type=jnp.float32)

        @pl.when(mine == 0)
        def _():
            rdma(part.at[slot], from_near.at[i // 2], near_send.at[half], near_recv.at[i // 2], r, near).start()

        @pl.when(jnp.logical_and(mine == 1, local == 0))
        def _():
            await_bytes(from_near.at[half], near_recv.at[half])
            part[slot] += from_near[half]
            for c in range(QB // CH):
                at = pl.ds(c * CH, CH)
                rdma(part.at[slot, at], from_far.at[half, at], far_send, far_recv.at[half, c], r, far).start()

        return carry

    lax.fori_loop(0, 8, block, 0)
    await_bytes(x_all.at[0], x_fwd_send)

    def h_rows(cp, tp, j):
        return h_ref.at[pl.ds(pl.multiple_of((cp * tp_size + tp) * rows + j * HC, HC), HC)]

    def h_block(cp, tp):
        return h_ref.at[pl.ds(pl.multiple_of((cp * tp_size + tp) * rows, rows), rows)]

    OWN, PEER, FAR, DIAG = range(4)
    h_chunks = rows // HC
    for j in range(h_chunks):
        first = j * HC
        half, within = first // QB, first % QB
        at = slice(within, within + HC)
        if within == 0:
            await_bytes(from_near.at[2 + half], near_recv.at[2 + half])
        if within % CH == 0:
            await_bytes(from_far.at[half, pl.ds(within, CH)], far_recv.at[half, within // CH])
        total = part[4 + half, at, :] + from_near[2 + half, at, :] + from_far[half, at, :]
        hbuf[first:first + HC, :] = (x_ref[first:first + HC, :].astype(jnp.float32) + total).astype(jnp.bfloat16)
        src = hbuf.at[pl.ds(first, HC)]
        mine = h_rows(r, t, j)
        rdma(src, mine, h_send, h_far.at[j], r, far).start()
        rdma(src, mine, h_send, h_peer.at[j], peer, t).start()
        rdma(src, mine, h_send, h_near.at[OWN], r, near).start()

    await_bytes(slots.at[pl.ds(0, num_devs - 1)], slot_recv)
    local_slots = (num_exp // num_devs) * cap

    def pick(n, dev, src):
        ids = slots[dev] - me * local_slots
        want = lax.broadcasted_iota(jnp.int32, (local_slots, rows), 0)
        sel = jnp.logical_or(ids[0:1, :] == want, ids[1:2, :] == want)
        sel = jnp.where(sel, 1.0, 0.0).astype(jnp.bfloat16)
        stage = x_all.at[2, pl.ds((n % 2) * local_slots, local_slots)]
        out = lambda k: [pltpu.make_async_copy(x_all.at[2, pl.ds((k % 2) * local_slots + e * cap, cap)], tok_ref.at[e, pl.ds(pl.multiple_of(dev * cap, cap), cap)], tok_sem.at[k % 2]) for e in range(num_exp // num_devs)]
        if n >= 2:
            await_bytes(stage, tok_sem.at[n % 2])
        for c0 in range(0, width, 512):
            stage[:, c0:c0 + 512] = jnp.dot(sel, src[:, c0:c0 + 512], preferred_element_type=jnp.float32).astype(jnp.bfloat16)
        for copy in out(n):
            copy.start()

    def fetch(n, cp, tp):
        return pltpu.make_async_copy(h_block(cp, tp), x_all.at[n % 2], load_sem.at[n % 2])

    def forward(got, kind):
        rdma(got, got, h_send, h_near.at[kind], r, near).start()

    pick(0, me, hbuf)
    for j in range(h_chunks):
        got = h_rows(peer, t, j)
        await_bytes(got, h_peer.at[j])
        forward(got, PEER)
    fetch(1, peer, t).start()
    fetch(1, peer, t).wait()
    pick(1, peer * tp_size + t, x_all.at[1])

    def diag(j):
        got = h_rows(peer, far, j)
        await_bytes(got, h_diag.at[j])
        forward(got, DIAG)

    for j in range(h_chunks):
        got = h_rows(r, far, j)
        await_bytes(got, h_far.at[j])
        rdma(got, got, h_send, h_diag.at[j], peer, t).start()
        forward(got, FAR)
        if j > 1:
            diag(j - 2)
        if j == 2:
            await_bytes(h_block(r, near), h_near.at[OWN])
            fetch(2, r, near).start()
            fetch(2, r, near).wait()
            pick(2, r * tp_size + near, x_all.at[0])
        if j == 4:
            await_bytes(h_block(peer, near), h_near.at[PEER])
            fetch(3, peer, near).start()
            fetch(3, peer, near).wait()
            pick(3, peer * tp_size + near, x_all.at[1])
    fetch(4, r, far).start()
    diag(h_chunks - 2)
    await_bytes(h_block(r, far_near), h_near.at[FAR])
    fetch(5, r, far_near).start()
    fetch(4, r, far).wait()
    pick(4, r * tp_size + far, x_all.at[0])
    fetch(5, r, far_near).wait()
    pick(5, r * tp_size + far_near, x_all.at[1])
    diag(h_chunks - 1)
    fetch(6, peer, far).start()
    await_bytes(h_block(peer, far_near), h_near.at[DIAG])
    fetch(7, peer, far_near).start()
    fetch(6, peer, far).wait()
    pick(6, peer * tp_size + far, x_all.at[0])
    fetch(7, peer, far_near).wait()
    pick(7, peer * tp_size + far_near, x_all.at[1])

    for n in range(2):
        await_bytes(x_all.at[2, pl.ds(0, local_slots)], tok_sem.at[n])
        await_bytes(part.at[n], near_send.at[n])
    await_bytes(h_ref.at[pl.ds(0, 7 * rows)], h_send)
    await_bytes(part.at[pl.ds(0, 2)], far_send)
    await_bytes(slots.at[pl.ds(0, num_devs - 1)], slot_send)
    await_bytes(x_all.at[pl.ds(0, 2)], x_send)
    await_bytes(kv_ref.at[pl.ds(0, tp_size * rows)], kv_send)


def moe_kernel(num_devs, tp_size, exp_local, cap, tok_ref, h_ref, slot_ref, gate_ref, wg_ref, wu_ref, wd_ref, y_ref, tok, wgb, wub, wdb, zrecv, yacc, cols, tsem, wsem, send_sem, recv_sem):
    rows, width = y_ref.shape
    local_slots = exp_local * cap
    me = lax.axis_index('cp') * tp_size + lax.axis_index('tp')
    groups = recv_sem.shape[0]
    per_group = exp_local // groups

    def weight_copies(e, slot):
        return [pltpu.make_async_copy(src.at[e], dst.at[slot], wsem.at[i, slot]) for i, (src, dst) in enumerate(((wg_ref, wgb), (wu_ref, wub), (wd_ref, wdb)))]

    loads = [pltpu.make_async_copy(tok_ref.at[at], tok.at[at], tsem.at[n]) for n, at in enumerate((pl.ds(0, 2), pl.ds(2, exp_local - 2)))]
    for e in range(2):
        loads[e].start()
        for copy in weight_copies(e, e):
            copy.start()
    greet([(lax.rem(me + j, num_devs) // tp_size, lax.rem(lax.rem(me + j, num_devs), tp_size)) for j in range(1, num_devs)])
    slot = slot_ref[0:2, :]
    back = (slot // cap % exp_local) * (num_devs * cap) + slot // local_slots * cap + slot % cap
    columns = jnp.concatenate([back.astype(jnp.float32), gate_ref[...], jnp.zeros((124, rows), jnp.float32)], axis=0)
    cols[...] = jnp.transpose(columns)
    yacc[...] = h_ref[...].astype(jnp.float32)
    loads[0].wait()

    def expert(e, carry):
        slot = lax.rem(e, 2)
        for copy in weight_copies(e, slot):
            copy.wait()

        @pl.when(e == 2)
        def _():
            loads[1].wait()

        x = tok[e]
        gate = jnp.dot(x, wgb[slot], preferred_element_type=jnp.float32)
        up = jnp.dot(x, wub[slot], preferred_element_type=jnp.float32)
        act = (jax.nn.silu(gate) * up).astype(jnp.bfloat16)
        tok[e] = jnp.dot(act, wdb[slot], preferred_element_type=jnp.float32).astype(jnp.bfloat16)
        group = e // per_group
        for j in range(1, num_devs):
            other = lax.rem(me + j, num_devs)
            rdma(tok.at[e, pl.ds(pl.multiple_of(other * cap, cap), cap)], zrecv.at[e, pl.ds(pl.multiple_of(me * cap, cap), cap)], send_sem, recv_sem.at[group], other // tp_size, lax.rem(other, tp_size)).start()
        at = pl.ds(pl.multiple_of(me * cap, cap), cap)
        zrecv[e, at, :] = tok[e, at, :]

        @pl.when(e + 2 < exp_local)
        def _():
            for copy in weight_copies(e + 2, slot):
                copy.start()

        return carry

    lax.fori_loop(0, exp_local, expert, 0)

    span = per_group * num_devs * cap

    def combine(g, carry):
        await_bytes(zrecv.at[pl.ds(0, per_group), pl.ds(0, (num_devs - 1) * cap)], recv_sem.at[g])
        want = (lax.broadcasted_iota(jnp.int32, (rows, span), 1) + g * span).astype(jnp.float32)
        sel0 = jnp.where(cols[:, 0:1] == want, 1.0, 0.0).astype(jnp.bfloat16)
        sel1 = jnp.where(cols[:, 1:2] == want, 1.0, 0.0).astype(jnp.bfloat16)
        first = pl.multiple_of(g * per_group, per_group)
        for c0 in range(0, width, 512):
            z = zrecv[pl.ds(first, per_group), :, c0:c0 + 512].reshape(span, 512)
            z0 = jnp.dot(sel0, z, preferred_element_type=jnp.float32)
            z1 = jnp.dot(sel1, z, preferred_element_type=jnp.float32)
            yacc[:, c0:c0 + 512] += cols[:, 2:3] * z0 + cols[:, 3:4] * z1
        return carry

    lax.fori_loop(0, groups, combine, 0)
    y_ref[...] = yacc[...].astype(y_ref.dtype)
    await_bytes(tok.at[:, pl.ds(0, (num_devs - 1) * cap)], send_sem)


def solution(mesh):
    cp_size = mesh.shape['cp']
    tp_size = mesh.shape['tp']
    num_devs = cp_size * tp_size
    row_spec = P(('data', 'cp', 'tp'), None)
    head_spec = P(None, 'tp', None)
    wo_spec = P('tp', None, None)
    expert_spec = P(('cp', 'tp'), None, None)

    vmem = pl.BlockSpec(memory_space=pltpu.VMEM)
    hbm = pl.BlockSpec(memory_space=pl.ANY)
    dma = pltpu.SemaphoreType.DMA
    bf16, f32 = jnp.bfloat16, jnp.float32

    def params(number):
        return pltpu.CompilerParams(collective_id=number, has_side_effects=True, vmem_limit_bytes=VLIM)

    def front(x_blk, idx, w_q, w_k, w_v, w_o, heads, hd, exp_local, cap):
        rows, width = x_blk.shape
        group = rows * tp_size
        v32 = lambda *shape: pltpu.VMEM(shape, f32)
        v16 = lambda *shape: pltpu.VMEM(shape, bf16)
        return pl.pallas_call(
            functools.partial(front_kernel, cp_size, tp_size, heads, hd, exp_local * num_devs, cap),
            in_specs=[vmem, vmem, hbm, hbm, hbm, hbm],
            out_specs=[hbm, hbm, vmem, vmem],
            out_shape=[jax.ShapeDtypeStruct((rows * num_devs, width), bf16), jax.ShapeDtypeStruct((exp_local, num_devs * cap, width), bf16), jax.ShapeDtypeStruct((rows, width), bf16), jax.ShapeDtypeStruct((8, rows), jnp.int32)],
            scratch_shapes=[
                v16(3, rows, width), v16(width, heads * hd), v16(width, 2 * hd), v16(heads * hd, width), v16(group, heads * hd), v16(group * cp_size, 2 * hd),
                pltpu.VMEM((num_devs, 8, rows), jnp.int32), v32(heads * QB, 128), v32(heads * QB, 128), v32(heads * QB, hd), v16(QB, heads * hd),
                v32(6, QB, width), v32(4, QB, width), v32(2, QB, width),
                dma((4,)), dma, dma, dma, dma, dma((rows // CH,)), dma, dma((rows // CH,)), dma, dma((2,)),
                dma((2,)), dma((4,)), dma, dma((2, QB // CH)), dma, dma((4,)), dma((rows // HC,)), dma((rows // HC,)), dma((rows // HC,)), dma((2,)), dma((2,))],
            compiler_params=params(0),
            name='front',
        )(x_blk, idx, w_q, w_k, w_v, w_o)

    def experts(tok, h_own, slots, gates, w_gate, w_up, w_down, cap):
        rows, width = h_own.shape
        exp_local, _, ff = w_gate.shape
        v16 = lambda *shape: pltpu.VMEM(shape, bf16)
        return pl.pallas_call(
            functools.partial(moe_kernel, num_devs, tp_size, exp_local, cap),
            in_specs=[hbm, vmem, vmem, vmem, hbm, hbm, hbm],
            out_specs=vmem,
            out_shape=jax.ShapeDtypeStruct((rows, width), bf16),
            scratch_shapes=[v16(exp_local, num_devs * cap, width), v16(2, width, ff), v16(2, width, ff), v16(2, ff, width), v16(exp_local, num_devs * cap, width), pltpu.VMEM((rows, width), f32), pltpu.VMEM((rows, 128), f32), dma((2,)), dma((3, 2)), dma, dma((4,))],
            compiler_params=params(1),
            name='moe',
        )(tok, h_own, slots, gates, w_gate, w_up, w_down)

    def device_fn(x_blk, w_q, w_k, w_v, w_o, idx_blk, gate_blk, w_gate, w_up, w_down):
        tok_dev, width = x_blk.shape
        heads, head_dim = w_q.shape[1], w_k.shape[2]
        exp_local = w_gate.shape[0]
        num_exp = exp_local * num_devs
        capacity = 4 * tok_dev // num_exp

        flat = lambda w: w.reshape(width, -1)
        _, tok, h_own, slots = front(x_blk, idx_blk.T, flat(w_q), flat(w_k), flat(w_v), w_o.reshape(heads * head_dim, width), heads, head_dim, exp_local, capacity)
        return experts(tok, h_own, slots, gate_blk.T, w_gate, w_up, w_down, capacity)

    return jax.shard_map(device_fn, mesh=mesh, in_specs=(row_spec, head_spec, head_spec, head_spec, wo_spec, row_spec, row_spec, expert_spec, expert_spec, expert_spec), out_specs=row_spec, check_vma=False)
```

```python
import functools
import jax
import jax.numpy as jnp
from jax import lax
from jax.experimental import pallas as pl
from jax.experimental.pallas import tpu as pltpu
from jax.sharding import PartitionSpec as P

QB = 256
KB = 512
CH = 128
HC = 64
XD = 2
WR = 256
LOG2E = 1.4426950408889634
VLIM = 60 * 1024 * 1024
MESH = pl.DeviceIdType.MESH


def attend_block(q_of, kv_ref, m_ref, l_ref, acc_ref, pos0, heads, hd):
    c = (hd ** -0.5) * LOG2E
    m_ref[...] = jnp.full(m_ref.shape, -jnp.inf, jnp.float32)
    l_ref[...] = jnp.zeros(l_ref.shape, jnp.float32)
    acc_ref[...] = jnp.zeros(acc_ref.shape, jnp.float32)

    def step(kb, masked):
        start = pl.multiple_of(kb * KB, KB)
        k = kv_ref[pl.ds(start, KB), :hd]
        v = kv_ref[pl.ds(start, KB), hd:]
        score = lambda h: lax.dot_general(q_of(h), k, (((1,), (1,)), ((), ())), preferred_element_type=jnp.float32)
        if masked:
            qp = pos0 + lax.broadcasted_iota(jnp.int32, (QB, KB), 0)
            kp = start + lax.broadcasted_iota(jnp.int32, (QB, KB), 1)
            keep = kp <= qp
        s_next = score(0)
        for h in range(heads):
            rows = slice(h * QB, (h + 1) * QB)
            s = s_next
            if h + 1 < heads:
                s_next = score(h + 1)
            if masked:
                s = jnp.where(keep, s, -jnp.inf)
            m_old = m_ref[rows, :]
            m_new = jnp.maximum(m_old, jnp.max(s, axis=1, keepdims=True))
            alpha = jnp.exp2((m_old - m_new) * c)
            p = jnp.exp2((s - jnp.concatenate([m_new] * (KB // 128), axis=1)) * c)
            lp = p[:, :128]
            for j in range(1, KB // 128):
                lp = lp + p[:, j * 128:(j + 1) * 128]
            m_ref[rows, :] = m_new
            l_ref[rows, :] = l_ref[rows, :] * alpha + lp
            acc_ref[rows, :] = acc_ref[rows, :] * alpha + jnp.dot(p.astype(jnp.bfloat16), v, preferred_element_type=jnp.float32)

    last = pos0 // KB

    def body(kb, carry):
        step(kb, False)
        return carry

    lax.fori_loop(0, last, body, 0)
    step(last, True)


def rdma(src, dst, send_sem, recv_sem, cp, tp):
    return pltpu.make_async_remote_copy(src_ref=src, dst_ref=dst, send_sem=send_sem, recv_sem=recv_sem, device_id=(0, cp, tp), device_id_type=MESH)


def await_bytes(ref, sem):
    pltpu.make_async_copy(ref, ref, sem).wait()


def greet(others):
    barrier = pltpu.get_barrier_semaphore()
    for cp, tp in others:
        pl.semaphore_signal(barrier, inc=1, device_id=(0, cp, tp), device_id_type=MESH)
    pl.semaphore_wait(barrier, len(others))


def slot_rows(idx_ref, num_exp, cap):
    rows = idx_ref.shape[1]
    expert = lax.broadcasted_iota(jnp.int32, (num_exp, rows), 0)
    hot = [jnp.where(idx_ref[k:k + 1, :] == expert, 1.0, 0.0) for k in range(2)]
    earlier = lax.broadcasted_iota(jnp.int32, (rows, rows), 0) < lax.broadcasted_iota(jnp.int32, (rows, rows), 1)
    earlier = jnp.where(earlier, 1.0, 0.0).astype(jnp.bfloat16)
    count = jnp.dot((hot[0] + hot[1]).astype(jnp.bfloat16), earlier, preferred_element_type=jnp.float32)
    return [idx_ref[k:k + 1, :] * cap + jnp.sum(hot[k] * count, axis=0, keepdims=True).astype(jnp.int32) for k in range(2)]


def front_kernel(cp_size, tp_size, heads, hd, num_exp, cap, x_ref, idx_ref, wq_ref, wk_ref, wv_ref, wo_ref, h_ref, tok_ref, hbuf, own_slots,
                 x_all, wq, wkv, wo, q_ref, kv_ref, slots, m_ref, l_ref, acc_ref, ob_ref, part, from_near, from_far,
                 wsem, slot_send, slot_recv, x_send, x_near, x_far, x_fwd_send, x_fwd, kv_send, kv_recv,
                 near_send, near_recv, far_send, far_recv, h_send, h_near, h_far, h_peer, h_diag, load_sem, tok_sem, raw, raw_sem):
    r, t = lax.axis_index('cp'), lax.axis_index('tp')
    num_devs = cp_size * tp_size
    me = r * tp_size + t
    near = t + 1 - 2 * lax.rem(t, 2)
    far = lax.rem(t + 2, tp_size)
    far_near = lax.rem(near + 2, tp_size)
    peer = 1 - r
    rows, width = x_ref.shape
    half_rows = rows // 2
    devs = [lax.rem(me + j, num_devs) for j in range(1, num_devs)]

    weights = [pltpu.make_async_copy(wk_ref, wkv.at[:, pl.ds(0, hd)], wsem.at[0]), pltpu.make_async_copy(wv_ref, wkv.at[:, pl.ds(hd, hd)], wsem.at[1]), pltpu.make_async_copy(wo_ref, wo, wsem.at[2])]
    for copy in weights:
        copy.start()

    def raw_copy(k, slot):
        return pltpu.make_async_copy(wq_ref.at[pl.ds(pl.multiple_of(k * WR, WR), WR)], raw.at[slot], raw_sem.at[slot])

    for k in range(2):
        raw_copy(k, k).start()
    greet([(d // tp_size, lax.rem(d, tp_size)) for d in devs])
    chunks = rows // CH
    for j in range(chunks):
        at = pl.ds(j * CH, CH)
        rdma(x_ref.at[at], x_all.at[0, at], x_send, x_far.at[j], r, far).start()
    rdma(x_ref, x_all.at[1], x_send, x_near, r, near).start()
    mine = slot_rows(idx_ref, num_exp, cap)
    own_slots[...] = jnp.concatenate(mine + [jnp.zeros((6, rows), jnp.int32)], axis=0)
    slots[me] = own_slots[...]
    for d in devs:
        rdma(own_slots, slots.at[me], slot_send, slot_recv, d // tp_size, lax.rem(d, tp_size)).start()
    for copy in weights[:2]:
        copy.wait()

    def flatten(k, carry):
        slot = lax.rem(k, 2)
        raw_copy(k, slot).wait()
        at = pl.ds(pl.multiple_of(k * WR, WR), WR)
        for h in range(heads):
            wq[at, h * hd:(h + 1) * hd] = raw[slot, :, h, :]

        @pl.when(k + 2 < width // WR)
        def _():
            raw_copy(k + 2, slot).start()

        return carry

    lax.fori_loop(0, width // WR, flatten, 0)

    def project(x, tp_src, row0, count):
        half = row0 // half_rows
        seg = r + half * (2 * cp_size - 1 - 2 * r)
        pos = pl.multiple_of((seg * tp_size + tp_src) * half_rows + row0 % half_rows, CH)
        kv_ref[pl.ds(pos, count), :] = jnp.dot(x, wkv[...], preferred_element_type=jnp.float32).astype(jnp.bfloat16)
        sent = kv_ref.at[pl.ds(pos, count)]
        rdma(sent, sent, kv_send, kv_recv.at[half], peer, t).start()
        at = pl.ds(pl.multiple_of(tp_src * rows + row0, CH), count)
        q_ref[at, :] = jnp.dot(x, wq[...], preferred_element_type=jnp.float32).astype(jnp.bfloat16)

    def project_far(half):
        for j in range(half * (chunks // 2), (half + 1) * (chunks // 2)):
            at = pl.ds(j * CH, CH)
            await_bytes(x_all.at[0, at], x_far.at[j])
            rdma(x_all.at[0, at], x_all.at[2, at], x_fwd_send, x_fwd.at[j], r, near).start()
            project(x_all[0, j * CH:(j + 1) * CH, :], far, j * CH, CH)
            await_bytes(x_all.at[2, at], x_fwd.at[j])
            project(x_all[2, j * CH:(j + 1) * CH, :], far_near, j * CH, CH)
        await_bytes(kv_ref.at[pl.ds(0, tp_size * half_rows)], kv_recv.at[half])

    for half in range(2):
        project(x_ref[half * half_rows:(half + 1) * half_rows, :], t, half * half_rows, half_rows)
    await_bytes(x_all.at[1], x_near)
    for half in range(2):
        project(x_all[1, half * half_rows:(half + 1) * half_rows, :], near, half * half_rows, half_rows)
    project_far(0)
    weights[2].wait()

    def h_rows(cp, tp, j):
        return h_ref.at[pl.ds(pl.multiple_of((cp * tp_size + tp) * rows + j * HC, HC), HC)]

    def h_block(cp, tp):
        return h_ref.at[pl.ds(pl.multiple_of((cp * tp_size + tp) * rows, rows), rows)]

    OWN, PEER, FAR, DIAG = range(4)
    h_chunks = rows // HC

    def finish(half):
        await_bytes(from_near.at[2 + half], near_recv.at[2 + half])
        for within in range(0, QB, HC):
            first = half * QB + within
            j = first // HC
            at = slice(within, within + HC)
            if within % CH == 0:
                await_bytes(from_far.at[half, pl.ds(within, CH)], far_recv.at[half, within // CH])
            total = part[4 + half, at, :] + from_near[2 + half, at, :] + from_far[half, at, :]
            hbuf[first:first + HC, :] = (x_ref[first:first + HC, :].astype(jnp.float32) + total).astype(jnp.bfloat16)
            src = hbuf.at[pl.ds(first, HC)]
            mine = h_rows(r, t, j)
            rdma(src, mine, h_send, h_far.at[j], r, far).start()
            rdma(src, mine, h_send, h_peer.at[j], peer, t).start()
            rdma(src, mine, h_send, h_near.at[OWN], r, near).start()

    def block(i, carry):
        local = i // 4
        mine = lax.rem(i, 2)
        half = lax.rem(i // 2, 2)
        slot = mine * (2 + 2 * local) + half

        @pl.when(i == 2)
        def _():
            project_far(1)

        @pl.when(i == 6)
        def _():
            finish(0)

        @pl.when(jnp.logical_and(mine == 0, local == 1))
        def _():
            await_bytes(part.at[half], near_send.at[half])

        t_dst = lax.rem(mine * t + (1 - mine) * near + 2 * (1 - local), tp_size)
        seg = r + half * (2 * cp_size - 1 - 2 * r)
        pos0 = (seg * tp_size + t_dst) * QB
        row0 = pl.multiple_of(t_dst * rows + half * QB, QB)
        attend_block(lambda h: q_ref[pl.ds(row0, QB), h * hd:(h + 1) * hd], kv_ref, m_ref, l_ref, acc_ref, pos0, heads, hd)
        for h in range(heads):
            at = slice(h * QB, (h + 1) * QB)
            den = jnp.sum(l_ref[at, :], axis=1, keepdims=True)
            ob_ref[:, h * hd:(h + 1) * hd] = (acc_ref[at, :] / den).astype(jnp.bfloat16)
        part[slot] = jnp.dot(ob_ref[...], wo[...], preferred_element_type=jnp.float32)

        @pl.when(mine == 0)
        def _():
            rdma(part.at[slot], from_near.at[i // 2], near_send.at[half], near_recv.at[i // 2], r, near).start()

        @pl.when(jnp.logical_and(mine == 1, local == 0))
        def _():
            await_bytes(from_near.at[half], near_recv.at[half])
            part[slot] += from_near[half]
            for c in range(QB // CH):
                at = pl.ds(c * CH, CH)
                rdma(part.at[slot, at], from_far.at[half, at], far_send, far_recv.at[half, c], r, far).start()

        return carry

    lax.fori_loop(0, 8, block, 0)
    await_bytes(x_all.at[0], x_fwd_send)

    finish(1)
    await_bytes(slots.at[pl.ds(0, num_devs - 1)], slot_recv)
    local_slots = (num_exp // num_devs) * cap

    def pick(n, dev, src):
        ids = slots[dev] - me * local_slots
        want = lax.broadcasted_iota(jnp.int32, (local_slots, rows), 0)
        sel = jnp.logical_or(ids[0:1, :] == want, ids[1:2, :] == want)
        sel = jnp.where(sel, 1.0, 0.0).astype(jnp.bfloat16)
        stage = x_all.at[2, pl.ds((n % 2) * local_slots, local_slots)]
        out = lambda k: [pltpu.make_async_copy(x_all.at[2, pl.ds((k % 2) * local_slots + e * cap, cap)], tok_ref.at[e, pl.ds(pl.multiple_of(dev * cap, cap), cap)], tok_sem.at[k % 2]) for e in range(num_exp // num_devs)]
        if n >= 2:
            await_bytes(stage, tok_sem.at[n % 2])
        for c0 in range(0, width, 512):
            stage[:, c0:c0 + 512] = jnp.dot(sel, src[:, c0:c0 + 512], preferred_element_type=jnp.float32).astype(jnp.bfloat16)
        for copy in out(n):
            copy.start()

    def fetch(n, cp, tp):
        return pltpu.make_async_copy(h_block(cp, tp), x_all.at[n % 2], load_sem.at[n % 2])

    def forward(got, kind):
        rdma(got, got, h_send, h_near.at[kind], r, near).start()

    def diag(j):
        got = h_rows(peer, far, j)
        await_bytes(got, h_diag.at[j])
        forward(got, DIAG)

    def from_peer(j):
        got = h_rows(peer, t, j)
        await_bytes(got, h_peer.at[j])
        forward(got, PEER)
        if j < XD:
            rdma(got, got, h_send, h_diag.at[j], r, far).start()

    def across(j):
        got = h_rows(r, far, j)
        await_bytes(got, h_far.at[j])
        forward(got, FAR)
        if j >= XD:
            rdma(got, got, h_send, h_diag.at[j], peer, t).start()

    for j in range(h_chunks // 2):
        from_peer(j)
    pick(0, me, hbuf)
    for j in range(h_chunks // 2):
        across(j)
        from_peer(h_chunks // 2 + j)
    fetch(1, peer, t).start()
    fetch(1, peer, t).wait()
    pick(1, peer * tp_size + t, x_all.at[1])
    across(4)
    diag(2)
    diag(3)
    await_bytes(h_block(r, near), h_near.at[OWN])
    fetch(2, r, near).start()
    fetch(2, r, near).wait()
    pick(2, r * tp_size + near, x_all.at[0])
    across(5)
    await_bytes(h_block(peer, near), h_near.at[PEER])
    fetch(3, peer, near).start()
    fetch(3, peer, near).wait()
    pick(3, peer * tp_size + near, x_all.at[1])
    across(6)
    diag(4)
    across(7)
    fetch(4, r, far).start()
    diag(5)
    await_bytes(h_block(r, far_near), h_near.at[FAR])
    fetch(5, r, far_near).start()
    fetch(4, r, far).wait()
    pick(4, r * tp_size + far, x_all.at[0])
    diag(6)
    fetch(5, r, far_near).wait()
    pick(5, r * tp_size + far_near, x_all.at[1])
    for j in range(XD):
        diag(j)
    diag(7)
    fetch(6, peer, far).start()
    await_bytes(h_block(peer, far_near), h_near.at[DIAG])
    fetch(7, peer, far_near).start()
    fetch(6, peer, far).wait()
    pick(6, peer * tp_size + far, x_all.at[0])
    fetch(7, peer, far_near).wait()
    pick(7, peer * tp_size + far_near, x_all.at[1])

    for n in range(2):
        await_bytes(x_all.at[2, pl.ds(0, local_slots)], tok_sem.at[n])
        await_bytes(part.at[n], near_send.at[n])
    await_bytes(h_ref.at[pl.ds(0, 7 * rows)], h_send)
    await_bytes(part.at[pl.ds(0, 2)], far_send)
    await_bytes(slots.at[pl.ds(0, num_devs - 1)], slot_send)
    await_bytes(x_all.at[pl.ds(0, 2)], x_send)
    await_bytes(kv_ref.at[pl.ds(0, tp_size * rows)], kv_send)


def moe_kernel(num_devs, tp_size, exp_local, cap, tok_ref, h_ref, slot_ref, gate_ref, wg_ref, wu_ref, wd_ref, y_ref, tok, wgb, wub, wdb, zrecv, yacc, cols, tsem, wsem, send_sem, recv_sem):
    rows, width = y_ref.shape
    local_slots = exp_local * cap
    me = lax.axis_index('cp') * tp_size + lax.axis_index('tp')
    groups = recv_sem.shape[0]
    per_group = exp_local // groups

    def weight_copies(e, slot):
        return [pltpu.make_async_copy(src.at[e], dst.at[slot], wsem.at[i, slot]) for i, (src, dst) in enumerate(((wg_ref, wgb), (wu_ref, wub), (wd_ref, wdb)))]

    loads = [pltpu.make_async_copy(tok_ref.at[at], tok.at[at], tsem.at[n]) for n, at in enumerate((pl.ds(0, 2), pl.ds(2, exp_local - 2)))]
    for e in range(2):
        loads[e].start()
        for copy in weight_copies(e, e):
            copy.start()
    greet([(lax.rem(me + j, num_devs) // tp_size, lax.rem(lax.rem(me + j, num_devs), tp_size)) for j in range(1, num_devs)])
    slot = slot_ref[0:2, :]
    back = (slot // cap % exp_local) * (num_devs * cap) + slot // local_slots * cap + slot % cap
    columns = jnp.concatenate([back.astype(jnp.float32), gate_ref[...], jnp.zeros((124, rows), jnp.float32)], axis=0)
    cols[...] = jnp.transpose(columns)
    yacc[...] = h_ref[...].astype(jnp.float32)
    loads[0].wait()

    def expert(e, carry):
        slot = lax.rem(e, 2)
        for copy in weight_copies(e, slot):
            copy.wait()

        @pl.when(e == 2)
        def _():
            loads[1].wait()

        x = tok[e]
        gate = jnp.dot(x, wgb[slot], preferred_element_type=jnp.float32)
        up = jnp.dot(x, wub[slot], preferred_element_type=jnp.float32)
        act = (jax.nn.silu(gate) * up).astype(jnp.bfloat16)
        tok[e] = jnp.dot(act, wdb[slot], preferred_element_type=jnp.float32).astype(jnp.bfloat16)
        group = e // per_group
        for j in range(1, num_devs):
            other = lax.rem(me + j, num_devs)
            rdma(tok.at[e, pl.ds(pl.multiple_of(other * cap, cap), cap)], zrecv.at[e, pl.ds(pl.multiple_of(me * cap, cap), cap)], send_sem, recv_sem.at[group], other // tp_size, lax.rem(other, tp_size)).start()
        at = pl.ds(pl.multiple_of(me * cap, cap), cap)
        zrecv[e, at, :] = tok[e, at, :]

        @pl.when(e + 2 < exp_local)
        def _():
            for copy in weight_copies(e + 2, slot):
                copy.start()

        return carry

    lax.fori_loop(0, exp_local, expert, 0)

    span = per_group * num_devs * cap

    def combine(g, carry):
        await_bytes(zrecv.at[pl.ds(0, per_group), pl.ds(0, (num_devs - 1) * cap)], recv_sem.at[g])
        want = (lax.broadcasted_iota(jnp.int32, (rows, span), 1) + g * span).astype(jnp.float32)
        sel0 = jnp.where(cols[:, 0:1] == want, 1.0, 0.0).astype(jnp.bfloat16)
        sel1 = jnp.where(cols[:, 1:2] == want, 1.0, 0.0).astype(jnp.bfloat16)
        first = pl.multiple_of(g * per_group, per_group)
        for c0 in range(0, width, 512):
            z = zrecv[pl.ds(first, per_group), :, c0:c0 + 512].reshape(span, 512)
            z0 = jnp.dot(sel0, z, preferred_element_type=jnp.float32)
            z1 = jnp.dot(sel1, z, preferred_element_type=jnp.float32)
            yacc[:, c0:c0 + 512] += cols[:, 2:3] * z0 + cols[:, 3:4] * z1
        return carry

    lax.fori_loop(0, groups, combine, 0)
    y_ref[...] = yacc[...].astype(y_ref.dtype)
    await_bytes(tok.at[:, pl.ds(0, (num_devs - 1) * cap)], send_sem)


def solution(mesh):
    cp_size = mesh.shape['cp']
    tp_size = mesh.shape['tp']
    num_devs = cp_size * tp_size
    row_spec = P(('data', 'cp', 'tp'), None)
    head_spec = P(None, 'tp', None)
    wo_spec = P('tp', None, None)
    expert_spec = P(('cp', 'tp'), None, None)

    vmem = pl.BlockSpec(memory_space=pltpu.VMEM)
    hbm = pl.BlockSpec(memory_space=pl.ANY)
    dma = pltpu.SemaphoreType.DMA
    bf16, f32 = jnp.bfloat16, jnp.float32

    def params(number):
        return pltpu.CompilerParams(collective_id=number, has_side_effects=True, vmem_limit_bytes=VLIM)

    def front(x_blk, idx, w_q, w_k, w_v, w_o, heads, hd, exp_local, cap):
        rows, width = x_blk.shape
        group = rows * tp_size
        v32 = lambda *shape: pltpu.VMEM(shape, f32)
        v16 = lambda *shape: pltpu.VMEM(shape, bf16)
        return pl.pallas_call(
            functools.partial(front_kernel, cp_size, tp_size, heads, hd, exp_local * num_devs, cap),
            in_specs=[vmem, vmem, hbm, hbm, hbm, hbm],
            out_specs=[hbm, hbm, vmem, vmem],
            out_shape=[jax.ShapeDtypeStruct((rows * num_devs, width), bf16), jax.ShapeDtypeStruct((exp_local, num_devs * cap, width), bf16), jax.ShapeDtypeStruct((rows, width), bf16), jax.ShapeDtypeStruct((8, rows), jnp.int32)],
            scratch_shapes=[
                v16(3, rows, width), v16(width, heads * hd), v16(width, 2 * hd), v16(heads * hd, width), v16(group, heads * hd), v16(group * cp_size, 2 * hd),
                pltpu.VMEM((num_devs, 8, rows), jnp.int32), v32(heads * QB, 128), v32(heads * QB, 128), v32(heads * QB, hd), v16(QB, heads * hd),
                v32(6, QB, width), v32(4, QB, width), v32(2, QB, width),
                dma((3,)), dma, dma, dma, dma, dma((rows // CH,)), dma, dma((rows // CH,)), dma, dma((2,)),
                dma((2,)), dma((4,)), dma, dma((2, QB // CH)), dma, dma((4,)), dma((rows // HC,)), dma((rows // HC,)), dma((rows // HC,)), dma((2,)), dma((2,)), v16(2, WR, heads, hd), dma((2,))],
            compiler_params=params(0),
            name='front',
        )(x_blk, idx, w_q, w_k, w_v, w_o)

    def experts(tok, h_own, slots, gates, w_gate, w_up, w_down, cap):
        rows, width = h_own.shape
        exp_local, _, ff = w_gate.shape
        v16 = lambda *shape: pltpu.VMEM(shape, bf16)
        return pl.pallas_call(
            functools.partial(moe_kernel, num_devs, tp_size, exp_local, cap),
            in_specs=[hbm, vmem, vmem, vmem, hbm, hbm, hbm],
            out_specs=vmem,
            out_shape=jax.ShapeDtypeStruct((rows, width), bf16),
            scratch_shapes=[v16(exp_local, num_devs * cap, width), v16(2, width, ff), v16(2, width, ff), v16(2, ff, width), v16(exp_local, num_devs * cap, width), pltpu.VMEM((rows, width), f32), pltpu.VMEM((rows, 128), f32), dma((2,)), dma((3, 2)), dma, dma((4,))],
            compiler_params=params(1),
            name='moe',
        )(tok, h_own, slots, gates, w_gate, w_up, w_down)

    def device_fn(x_blk, w_q, w_k, w_v, w_o, idx_blk, gate_blk, w_gate, w_up, w_down):
        tok_dev, width = x_blk.shape
        heads, head_dim = w_q.shape[1], w_k.shape[2]
        exp_local = w_gate.shape[0]
        num_exp = exp_local * num_devs
        capacity = 4 * tok_dev // num_exp

        flat = lambda w: w.reshape(width, -1)
        _, tok, h_own, slots = front(x_blk, idx_blk.T, w_q, flat(w_k), flat(w_v), w_o.reshape(heads * head_dim, width), heads, head_dim, exp_local, capacity)
        return experts(tok, h_own, slots, gate_blk.T, w_gate, w_up, w_down, capacity)

    return jax.shard_map(device_fn, mesh=mesh, in_specs=(row_spec, head_spec, head_spec, head_spec, wo_spec, row_spec, row_spec, expert_spec, expert_spec, expert_spec), out_specs=row_spec, check_vma=False)
```

```python
import functools
import jax
import jax.numpy as jnp
from jax import lax
from jax.experimental import pallas as pl
from jax.experimental.pallas import tpu as pltpu
from jax.sharding import PartitionSpec as P

QB = 256
KB = 512
CH = 128
HC = 64
OVER_X = (7,)
OV = 32
LIMIT = OV
WR = 256
LOG2E = 1.4426950408889634
VLIM = 60 * 1024 * 1024
MESH = pl.DeviceIdType.MESH


def attend_block(q_of, kv_ref, m_ref, l_ref, acc_ref, pos0, heads, hd):
    c = (hd ** -0.5) * LOG2E
    m_ref[...] = jnp.full(m_ref.shape, -jnp.inf, jnp.float32)
    l_ref[...] = jnp.zeros(l_ref.shape, jnp.float32)
    acc_ref[...] = jnp.zeros(acc_ref.shape, jnp.float32)

    def step(kb, masked):
        start = pl.multiple_of(kb * KB, KB)
        k = kv_ref[pl.ds(start, KB), :hd]
        v = kv_ref[pl.ds(start, KB), hd:]
        score = lambda h: lax.dot_general(q_of(h), k, (((1,), (1,)), ((), ())), preferred_element_type=jnp.float32)
        if masked:
            qp = pos0 + lax.broadcasted_iota(jnp.int32, (QB, KB), 0)
            kp = start + lax.broadcasted_iota(jnp.int32, (QB, KB), 1)
            keep = kp <= qp
        s_next = score(0)
        for h in range(heads):
            rows = slice(h * QB, (h + 1) * QB)
            s = s_next
            if h + 1 < heads:
                s_next = score(h + 1)
            if masked:
                s = jnp.where(keep, s, -jnp.inf)
            m_old = m_ref[rows, :]
            m_new = jnp.maximum(m_old, jnp.max(s, axis=1, keepdims=True))
            alpha = jnp.exp2((m_old - m_new) * c)
            p = jnp.exp2((s - jnp.concatenate([m_new] * (KB // 128), axis=1)) * c)
            lp = p[:, :128]
            for j in range(1, KB // 128):
                lp = lp + p[:, j * 128:(j + 1) * 128]
            m_ref[rows, :] = m_new
            l_ref[rows, :] = l_ref[rows, :] * alpha + lp
            acc_ref[rows, :] = acc_ref[rows, :] * alpha + jnp.dot(p.astype(jnp.bfloat16), v, preferred_element_type=jnp.float32)

    last = pos0 // KB

    def body(kb, carry):
        step(kb, False)
        return carry

    lax.fori_loop(0, last, body, 0)
    step(last, True)


def rdma(src, dst, send_sem, recv_sem, cp, tp):
    return pltpu.make_async_remote_copy(src_ref=src, dst_ref=dst, send_sem=send_sem, recv_sem=recv_sem, device_id=(0, cp, tp), device_id_type=MESH)


def await_bytes(ref, sem):
    pltpu.make_async_copy(ref, ref, sem).wait()


def greet(others):
    barrier = pltpu.get_barrier_semaphore()
    for cp, tp in others:
        pl.semaphore_signal(barrier, inc=1, device_id=(0, cp, tp), device_id_type=MESH)
    pl.semaphore_wait(barrier, len(others))


def slot_rows(idx_ref, num_exp, exp_local, cap):
    rows = idx_ref.shape[1]
    expert = lax.broadcasted_iota(jnp.int32, (num_exp, rows), 0)
    hot = [jnp.where(idx_ref[k:k + 1, :] == expert, 1.0, 0.0) for k in range(2)]
    earlier = lax.broadcasted_iota(jnp.int32, (rows, rows), 0) < lax.broadcasted_iota(jnp.int32, (rows, rows), 1)
    earlier = jnp.where(earlier, 1.0, 0.0).astype(jnp.bfloat16)
    count = jnp.dot((hot[0] + hot[1]).astype(jnp.bfloat16), earlier, preferred_element_type=jnp.float32)
    lane_sum = jnp.sum(hot[0] + hot[1], axis=1, keepdims=True)
    over = jnp.maximum(lane_sum - cap // 2, 0.0)
    e0 = lax.broadcasted_iota(jnp.int32, (num_exp, num_exp), 0)
    e1 = lax.broadcasted_iota(jnp.int32, (num_exp, num_exp), 1)
    before = jnp.where(jnp.logical_and(e0 // exp_local == e1 // exp_local, e1 < e0), 1.0, 0.0).astype(jnp.bfloat16)
    offset = jnp.dot(before, jnp.broadcast_to(over, (num_exp, num_exp)).astype(jnp.bfloat16), preferred_element_type=jnp.float32)[:, 0:1]
    worst = jnp.broadcast_to(jnp.max(offset + over, axis=0, keepdims=True), (1, rows)).astype(jnp.int32)
    slots, ranks = [], []
    for k in range(2):
        pos = jnp.sum(hot[k] * count, axis=0, keepdims=True)
        rank = jnp.sum(hot[k] * offset, axis=0, keepdims=True) + pos - cap // 2
        slots.append(idx_ref[k:k + 1, :] * cap + pos.astype(jnp.int32))
        ranks.append(jnp.where(pos >= cap // 2, rank, -1.0).astype(jnp.int32))
    return slots + ranks + [worst]


def front_kernel(cp_size, tp_size, heads, hd, num_exp, cap, x_ref, idx_ref, wq_ref, wk_ref, wv_ref, wo_ref, h_ref, tok_ref, hbuf, own_slots, slots,
                 x_all, wq, wkv, wo, q_ref, kv_ref, m_ref, l_ref, acc_ref, ob_ref, part, from_near, from_far,
                 wsem, slot_send, slot_recv, x_send, x_near, x_far, x_fwd_send, x_fwd, kv_send, kv_recv,
                 near_send, near_recv, far_send, far_recv, h_send, h_near, h_far, h_peer, h_diag, load_sem, tok_sem, raw, raw_sem):
    r, t = lax.axis_index('cp'), lax.axis_index('tp')
    num_devs = cp_size * tp_size
    me = r * tp_size + t
    near = t + 1 - 2 * lax.rem(t, 2)
    far = lax.rem(t + 2, tp_size)
    far_near = lax.rem(near + 2, tp_size)
    peer = 1 - r
    rows, width = x_ref.shape
    half_rows = rows // 2
    devs = [lax.rem(me + j, num_devs) for j in range(1, num_devs)]

    weights = [pltpu.make_async_copy(wk_ref, wkv.at[:, pl.ds(0, hd)], wsem.at[0]), pltpu.make_async_copy(wv_ref, wkv.at[:, pl.ds(hd, hd)], wsem.at[1]), pltpu.make_async_copy(wo_ref, wo, wsem.at[2])]
    for copy in weights:
        copy.start()

    def raw_copy(k, slot):
        return pltpu.make_async_copy(wq_ref.at[pl.ds(pl.multiple_of(k * WR, WR), WR)], raw.at[slot], raw_sem.at[slot])

    for k in range(2):
        raw_copy(k, k).start()
    greet([(d // tp_size, lax.rem(d, tp_size)) for d in devs])
    chunks = rows // CH
    for j in range(chunks):
        at = pl.ds(j * CH, CH)
        rdma(x_ref.at[at], x_all.at[0, at], x_send, x_far.at[j], r, far).start()
    rdma(x_ref, x_all.at[1], x_send, x_near, r, near).start()
    mine = slot_rows(idx_ref, num_exp, num_exp // num_devs, cap)
    own_slots[...] = jnp.concatenate(mine + [jnp.zeros((3, rows), jnp.int32)], axis=0)
    slots[me] = own_slots[...]
    for d in devs:
        rdma(own_slots, slots.at[me], slot_send, slot_recv, d // tp_size, lax.rem(d, tp_size)).start()
    for copy in weights[:2]:
        copy.wait()

    def flatten(k, carry):
        slot = lax.rem(k, 2)
        raw_copy(k, slot).wait()
        at = pl.ds(pl.multiple_of(k * WR, WR), WR)
        for h in range(heads):
            wq[at, h * hd:(h + 1) * hd] = raw[slot, :, h, :]

        @pl.when(k + 2 < width // WR)
        def _():
            raw_copy(k + 2, slot).start()

        return carry

    lax.fori_loop(0, width // WR, flatten, 0)

    def project(x, tp_src, row0, count):
        half = row0 // half_rows
        seg = r + half * (2 * cp_size - 1 - 2 * r)
        pos = pl.multiple_of((seg * tp_size + tp_src) * half_rows + row0 % half_rows, CH)
        kv_ref[pl.ds(pos, count), :] = jnp.dot(x, wkv[...], preferred_element_type=jnp.float32).astype(jnp.bfloat16)
        sent = kv_ref.at[pl.ds(pos, count)]
        rdma(sent, sent, kv_send, kv_recv.at[half], peer, t).start()
        at = pl.ds(pl.multiple_of(tp_src * rows + row0, CH), count)
        q_ref[at, :] = jnp.dot(x, wq[...], preferred_element_type=jnp.float32).astype(jnp.bfloat16)

    def project_far(half):
        for j in range(half * (chunks // 2), (half + 1) * (chunks // 2)):
            at = pl.ds(j * CH, CH)
            await_bytes(x_all.at[0, at], x_far.at[j])
            rdma(x_all.at[0, at], x_all.at[2, at], x_fwd_send, x_fwd.at[j], r, near).start()
            project(x_all[0, j * CH:(j + 1) * CH, :], far, j * CH, CH)
            await_bytes(x_all.at[2, at], x_fwd.at[j])
            project(x_all[2, j * CH:(j + 1) * CH, :], far_near, j * CH, CH)
        await_bytes(kv_ref.at[pl.ds(0, tp_size * half_rows)], kv_recv.at[half])

    for half in range(2):
        project(x_ref[half * half_rows:(half + 1) * half_rows, :], t, half * half_rows, half_rows)
    await_bytes(x_all.at[1], x_near)
    for half in range(2):
        project(x_all[1, half * half_rows:(half + 1) * half_rows, :], near, half * half_rows, half_rows)
    project_far(0)
    weights[2].wait()

    def h_rows(cp, tp, j):
        return h_ref.at[pl.ds(pl.multiple_of((cp * tp_size + tp) * rows + j * HC, HC), HC)]

    def h_block(cp, tp):
        return h_ref.at[pl.ds(pl.multiple_of((cp * tp_size + tp) * rows, rows), rows)]

    OWN, PEER, FAR, DIAG = range(4)
    h_chunks = rows // HC

    def finish(half):
        await_bytes(from_near.at[2 + half], near_recv.at[2 + half])
        for within in range(0, QB, HC):
            first = half * QB + within
            j = first // HC
            at = slice(within, within + HC)
            if within % CH == 0:
                await_bytes(from_far.at[half, pl.ds(within, CH)], far_recv.at[half, within // CH])
            total = part[4 + half, at, :] + from_near[2 + half, at, :] + from_far[half, at, :]
            hbuf[first:first + HC, :] = (x_ref[first:first + HC, :].astype(jnp.float32) + total).astype(jnp.bfloat16)
            src = hbuf.at[pl.ds(first, HC)]
            mine = h_rows(r, t, j)
            rdma(src, mine, h_send, h_far.at[j], r, far).start()
            rdma(src, mine, h_send, h_peer.at[j], peer, t).start()
            rdma(src, mine, h_send, h_near.at[OWN], r, near).start()

    def forward(got, kind):
        rdma(got, got, h_send, h_near.at[kind], r, near).start()

    def diag(j):
        got = h_rows(peer, far, j)
        await_bytes(got, h_diag.at[j])
        forward(got, DIAG)

    def from_peer(j):
        got = h_rows(peer, t, j)
        await_bytes(got, h_peer.at[j])
        forward(got, PEER)
        if j in OVER_X:
            rdma(got, got, h_send, h_diag.at[j], r, far).start()

    def across(j):
        got = h_rows(r, far, j)
        await_bytes(got, h_far.at[j])
        forward(got, FAR)
        if j not in OVER_X:
            rdma(got, got, h_send, h_diag.at[j], peer, t).start()

    def block(i, carry):
        half = i // 4
        local = lax.rem(i // 2, 2)
        mine = lax.rem(i, 2)
        slot = mine * (2 + 2 * local) + half

        @pl.when(i == 4)
        def _():
            project_far(1)

        @pl.when(i == 5)
        def _():
            finish(0)

        @pl.when(i == 7)
        def _():
            for j in range(h_chunks // 2):
                from_peer(j)
            for j in range(h_chunks // 2):
                across(j)

        @pl.when(jnp.logical_and(mine == 0, local == 1))
        def _():
            await_bytes(part.at[half], near_send.at[half])

        t_dst = lax.rem(mine * t + (1 - mine) * near + 2 * (1 - local), tp_size)
        seg = r + half * (2 * cp_size - 1 - 2 * r)
        pos0 = (seg * tp_size + t_dst) * QB
        row0 = pl.multiple_of(t_dst * rows + half * QB, QB)
        attend_block(lambda h: q_ref[pl.ds(row0, QB), h * hd:(h + 1) * hd], kv_ref, m_ref, l_ref, acc_ref, pos0, heads, hd)
        for h in range(heads):
            at = slice(h * QB, (h + 1) * QB)
            den = jnp.sum(l_ref[at, :], axis=1, keepdims=True)
            ob_ref[:, h * hd:(h + 1) * hd] = (acc_ref[at, :] / den).astype(jnp.bfloat16)
        part[slot] = jnp.dot(ob_ref[...], wo[...], preferred_element_type=jnp.float32)

        @pl.when(mine == 0)
        def _():
            rdma(part.at[slot], from_near.at[2 * local + half], near_send.at[half], near_recv.at[2 * local + half], r, near).start()

        @pl.when(jnp.logical_and(mine == 1, local == 0))
        def _():
            await_bytes(from_near.at[half], near_recv.at[half])
            part[slot] += from_near[half]
            for c in range(QB // CH):
                at = pl.ds(c * CH, CH)
                rdma(part.at[slot, at], from_far.at[half, at], far_send, far_recv.at[half, c], r, far).start()

        return carry

    lax.fori_loop(0, 8, block, 0)
    await_bytes(x_all.at[0], x_fwd_send)

    finish(1)
    await_bytes(slots.at[pl.ds(0, num_devs - 1)], slot_recv)
    local_slots = (num_exp // num_devs) * cap

    def pick(pair, ends):
        exp_local = num_exp // num_devs
        sels = []
        for dev, _ in ends:
            ids = slots[dev] - me * local_slots
            want = lax.broadcasted_iota(jnp.int32, (local_slots, rows), 0)
            sel = jnp.logical_or(ids[0:1, :] == want, ids[1:2, :] == want)
            sels.append(jnp.where(sel, 1.0, 0.0).astype(jnp.bfloat16))
        if pair > 0:
            await_bytes(x_all.at[2], tok_sem)
        for c0 in range(0, width, 512):
            parts = [jnp.dot(sel, src[:, c0:c0 + 512], preferred_element_type=jnp.float32).reshape(exp_local, 2, cap // 2, 512) for sel, (_, src) in zip(sels, ends)]
            x_all[2, :, c0:c0 + 512] = jnp.concatenate(parts, axis=2).reshape(rows, 512).astype(jnp.bfloat16)
        for e in range(exp_local):
            for upper in range(2):
                pltpu.make_async_copy(x_all.at[2, pl.ds((2 * e + upper) * cap, cap)], tok_ref.at[e, pl.ds(upper * (num_devs * cap // 2) + pair * cap, cap)], tok_sem).start()

    def fetch(n, cp, tp):
        return pltpu.make_async_copy(h_block(cp, tp), x_all.at[n % 2], load_sem.at[n % 2])

    for j in range(h_chunks // 2):
        diag(j)
    from_peer(4)
    across(4)
    await_bytes(h_block(r, near), h_near.at[OWN])
    fetch(1, r, near).start()
    fetch(1, r, near).wait()
    pick(0, ((me, hbuf), (r * tp_size + near, x_all.at[1])))
    for j in range(5, h_chunks):
        from_peer(j)
        across(j)
    fetch(0, peer, t).start()
    await_bytes(h_block(peer, near), h_near.at[PEER])
    fetch(1, peer, near).start()
    fetch(0, peer, t).wait()
    fetch(1, peer, near).wait()
    pick(1, ((peer * tp_size + t, x_all.at[0]), (peer * tp_size + near, x_all.at[1])))
    fetch(0, r, far).start()
    await_bytes(h_block(r, far_near), h_near.at[FAR])
    fetch(1, r, far_near).start()
    fetch(0, r, far).wait()
    fetch(1, r, far_near).wait()
    pick(2, ((r * tp_size + far, x_all.at[0]), (r * tp_size + far_near, x_all.at[1])))
    for j in range(4, h_chunks):
        diag(j)
    fetch(0, peer, far).start()
    await_bytes(h_block(peer, far_near), h_near.at[DIAG])
    fetch(1, peer, far_near).start()
    fetch(0, peer, far).wait()
    fetch(1, peer, far_near).wait()
    pick(3, ((peer * tp_size + far, x_all.at[0]), (peer * tp_size + far_near, x_all.at[1])))

    await_bytes(x_all.at[2], tok_sem)
    for n in range(2):
        await_bytes(part.at[n], near_send.at[n])
    await_bytes(h_ref.at[pl.ds(0, 7 * rows)], h_send)
    await_bytes(part.at[pl.ds(0, 2)], far_send)
    await_bytes(slots.at[pl.ds(0, num_devs - 1)], slot_send)
    await_bytes(x_all.at[pl.ds(0, 2)], x_send)
    await_bytes(kv_ref.at[pl.ds(0, tp_size * rows)], kv_send)


def moe_kernel(num_devs, tp_size, exp_local, cap, full, tok_ref, h_ref, slot_ref, slots_ref, gate_ref, wg_ref, wu_ref, wd_ref, y_ref, tok, wgb, wub, wdb, zrecv, over, yacc, cols, tsem, wsem, send_sem, over_sem, recv_sem):
    rows, width = y_ref.shape
    r, t = lax.axis_index('cp'), lax.axis_index('tp')
    me = r * tp_size + t
    near = t + 1 - 2 * lax.rem(t, 2)
    places = [(cp, lax.rem(tp + 2 * across, tp_size)) for across in range(2) for cp in (r, 1 - r) for tp in (t, near)]
    low = cap // 2
    pairs = exp_local // 2
    block = num_devs * cap
    half_block = block // 2

    def weight_copies(e, slot):
        return [pltpu.make_async_copy(src.at[e], dst.at[slot], wsem.at[i, slot]) for i, (src, dst) in enumerate(((wg_ref, wgb), (wu_ref, wub), (wd_ref, wdb)))]

    loads = [pltpu.make_async_copy(tok_ref.at[at], tok.at[at], tsem.at[n]) for n, at in enumerate((pl.ds(0, 2), pl.ds(2, exp_local - 2)))]
    for e in range(2):
        loads[e].start()
        for copy in weight_copies(e, e):
            copy.start()
    greet(places[1:])
    slot = slot_ref[0:2, :]
    pos = slot % cap
    expert = slot // cap
    dev = expert // exp_local
    el = expert % exp_local
    dev_cp, dev_tp = dev // tp_size, dev % tp_size
    place = jnp.where(dev_tp % 2 == t % 2, 0, 1) + jnp.where(dev_cp == r, 0, 2) + jnp.where(dev_tp // 2 == t // 2, 0, 4)
    home = (el // 2) * block + place * cap + (el % 2) * low + pos % low
    upper = pairs * block + (home if full else place * OV + slot_ref[2:4, :])
    back = jnp.where(pos < low, home, upper)
    columns = jnp.concatenate([back.astype(jnp.float32), gate_ref[...], jnp.zeros((124, rows), jnp.float32)], axis=0)
    cols[...] = jnp.transpose(columns)
    yacc[...] = h_ref[...].astype(jnp.float32)
    loads[0].wait()

    def send(src, dst, sem, group, n):
        rdma(src, dst, sem, recv_sem.at[group], *places[n]).start()

    def two_experts(m, carry):
        @pl.when(m == 1)
        def _():
            loads[1].wait()

        outs = []
        for b in range(2):
            e = 2 * m + b
            for copy in weight_copies(e, b):
                copy.wait()
            x = tok[e]
            gate = jnp.dot(x, wgb[b], preferred_element_type=jnp.float32)
            up = jnp.dot(x, wub[b], preferred_element_type=jnp.float32)
            act = (jax.nn.silu(gate) * up).astype(jnp.bfloat16)
            outs.append(jnp.dot(act, wdb[b], preferred_element_type=jnp.float32))

            @pl.when(e + 2 < exp_local)
            def _():
                for copy in weight_copies(e + 2, b):
                    copy.start()

        for side in range(2):
            pieces = [z[side * half_block:(side + 1) * half_block].reshape(num_devs, low, width) for z in outs]
            tok[2 * m + side] = jnp.concatenate(pieces, axis=1).reshape(block, width).astype(jnp.bfloat16)
            if side == 0 or full:
                at = side * pairs + m
                for n in range(1, num_devs):
                    part = pl.ds(n * cap, cap)
                    send(tok.at[2 * m + side, part], zrecv.at[at, part], over_sem if side else send_sem, at // 2, n)
                zrecv[at, :cap, :] = tok[2 * m + side, :cap, :]
        return carry

    lax.fori_loop(0, pairs, two_experts, 0)

    if not full:
        per_block = block // OV
        for n in (4, 5, 6, 7, 2, 3, 1, 0):
            cp, tp = places[n]
            ids = slots_ref[cp * tp_size + tp]
            mix = jnp.zeros((OV, half_block), jnp.float32)
            for k in range(2):
                own = ids[k:k + 1, :] - me * exp_local * cap
                inside = jnp.logical_and(own >= 0, own < exp_local * cap)
                spot = jnp.where(jnp.logical_and(inside, own % cap >= low), own // cap * low + own % cap - low, -1)
                a = jnp.where(ids[2 + k:3 + k, :] == lax.broadcasted_iota(jnp.int32, (OV, rows), 0), 1.0, 0.0).astype(jnp.bfloat16)
                b = jnp.where(spot == lax.broadcasted_iota(jnp.int32, (half_block * 2, rows), 0), 1.0, 0.0).astype(jnp.bfloat16)
                mix = lax.dot_general(a, b, (((1,), (1,)), ((), ())), preferred_element_type=jnp.float32) + (mix if k else 0.0)
            mix = mix.astype(jnp.bfloat16)
            for c0 in range(0, width, 512):
                z = jnp.concatenate([tok[2 * m + 1, n * cap:(n + 1) * cap, c0:c0 + 512] for m in range(pairs)], axis=0)
                over[n, :, c0:c0 + 512] = jnp.dot(mix, z, preferred_element_type=jnp.float32).astype(jnp.bfloat16)
            dst = zrecv.at[pairs + n // per_block, pl.ds(n % per_block * OV, OV)]
            if n:
                send(over.at[n], dst, over_sem, pairs // 2, n)
            else:
                dst[...] = over[n]

    groups = recv_sem.shape[0]
    span = 2 * block

    def combine(g, carry):
        await_bytes(zrecv.at[pl.ds(0, 2), pl.ds(0, (num_devs - 1) * cap)], recv_sem.at[g])
        want = (lax.broadcasted_iota(jnp.int32, (rows, span), 1) + g * span).astype(jnp.float32)
        sel0 = jnp.where(cols[:, 0:1] == want, 1.0, 0.0).astype(jnp.bfloat16)
        sel1 = jnp.where(cols[:, 1:2] == want, 1.0, 0.0).astype(jnp.bfloat16)
        first = pl.multiple_of(g * 2, 2)
        for c0 in range(0, width, 512):
            z = zrecv[pl.ds(first, 2), :, c0:c0 + 512].reshape(span, 512)
            z0 = jnp.dot(sel0, z, preferred_element_type=jnp.float32)
            z1 = jnp.dot(sel1, z, preferred_element_type=jnp.float32)
            yacc[:, c0:c0 + 512] += cols[:, 2:3] * z0 + cols[:, 3:4] * z1
        return carry

    lax.fori_loop(0, groups, combine, 0)
    y_ref[...] = yacc[...].astype(y_ref.dtype)
    await_bytes(tok.at[pl.ds(0, pairs), pl.ds(0, (num_devs - 1) * cap)], send_sem)
    await_bytes(tok.at[pl.ds(0, pairs if full else 2), pl.ds(0, (num_devs - 1) * cap)], over_sem)


def solution(mesh):
    cp_size = mesh.shape['cp']
    tp_size = mesh.shape['tp']
    num_devs = cp_size * tp_size
    row_spec = P(('data', 'cp', 'tp'), None)
    head_spec = P(None, 'tp', None)
    wo_spec = P('tp', None, None)
    expert_spec = P(('cp', 'tp'), None, None)

    vmem = pl.BlockSpec(memory_space=pltpu.VMEM)
    hbm = pl.BlockSpec(memory_space=pl.ANY)
    dma = pltpu.SemaphoreType.DMA
    bf16, f32 = jnp.bfloat16, jnp.float32

    def params(number):
        return pltpu.CompilerParams(collective_id=number, has_side_effects=True, vmem_limit_bytes=VLIM)

    def front(x_blk, idx, w_q, w_k, w_v, w_o, heads, hd, exp_local, cap):
        rows, width = x_blk.shape
        group = rows * tp_size
        v32 = lambda *shape: pltpu.VMEM(shape, f32)
        v16 = lambda *shape: pltpu.VMEM(shape, bf16)
        return pl.pallas_call(
            functools.partial(front_kernel, cp_size, tp_size, heads, hd, exp_local * num_devs, cap),
            in_specs=[vmem, vmem, hbm, hbm, hbm, hbm],
            out_specs=[hbm, hbm, vmem, vmem, vmem],
            out_shape=[jax.ShapeDtypeStruct((rows * num_devs, width), bf16), jax.ShapeDtypeStruct((exp_local, num_devs * cap, width), bf16), jax.ShapeDtypeStruct((rows, width), bf16), jax.ShapeDtypeStruct((8, rows), jnp.int32), jax.ShapeDtypeStruct((num_devs, 8, rows), jnp.int32)],
            scratch_shapes=[
                v16(3, rows, width), v16(width, heads * hd), v16(width, 2 * hd), v16(heads * hd, width), v16(group, heads * hd), v16(group * cp_size, 2 * hd),
                v32(heads * QB, 128), v32(heads * QB, 128), v32(heads * QB, hd), v16(QB, heads * hd),
                v32(6, QB, width), v32(4, QB, width), v32(2, QB, width),
                dma((3,)), dma, dma, dma, dma, dma((rows // CH,)), dma, dma((rows // CH,)), dma, dma((2,)),
                dma((2,)), dma((4,)), dma, dma((2, QB // CH)), dma, dma((4,)), dma((rows // HC,)), dma((rows // HC,)), dma((rows // HC,)), dma((2,)), dma, v16(2, WR, heads, hd), dma((2,))],
            compiler_params=params(0),
            name='front',
        )(x_blk, idx, w_q, w_k, w_v, w_o)

    def experts(full, cap, tok, h_own, own_slots, slots, gates, w_gate, w_up, w_down):
        rows, width = h_own.shape
        exp_local, _, ff = w_gate.shape
        v16 = lambda *shape: pltpu.VMEM(shape, bf16)
        block = num_devs * cap
        blocks = exp_local if full else exp_local // 2 + num_devs * OV // block
        return pl.pallas_call(
            functools.partial(moe_kernel, num_devs, tp_size, exp_local, cap, full),
            in_specs=[hbm, vmem, vmem, vmem, vmem, hbm, hbm, hbm],
            out_specs=vmem,
            out_shape=jax.ShapeDtypeStruct((rows, width), bf16),
            scratch_shapes=[v16(exp_local, block, width), v16(2, width, ff), v16(2, width, ff), v16(2, ff, width), v16(blocks, block, width), v16(num_devs, OV, width), pltpu.VMEM((rows, width), f32), pltpu.VMEM((rows, 128), f32), dma((2,)), dma((3, 2)), dma, dma, dma((blocks // 2,))],
            compiler_params=params(2 if full else 1),
            name='moe_full' if full else 'moe',
        )(tok, h_own, own_slots, slots, gates, w_gate, w_up, w_down)

    def device_fn(x_blk, w_q, w_k, w_v, w_o, idx_blk, gate_blk, w_gate, w_up, w_down):
        tok_dev, width = x_blk.shape
        heads, head_dim = w_q.shape[1], w_k.shape[2]
        exp_local = w_gate.shape[0]
        num_exp = exp_local * num_devs
        capacity = 4 * tok_dev // num_exp

        flat = lambda w: w.reshape(width, -1)
        _, tok, h_own, own_slots, slots = front(x_blk, idx_blk.T, w_q, flat(w_k), flat(w_v), w_o.reshape(heads * head_dim, width), heads, head_dim, exp_local, capacity)
        few = jnp.max(slots[:, 4, 0]) <= LIMIT
        return lax.cond(few, functools.partial(experts, False, capacity), functools.partial(experts, True, capacity), tok, h_own, own_slots, slots, gate_blk.T, w_gate, w_up, w_down)

    return jax.shard_map(device_fn, mesh=mesh, in_specs=(row_spec, head_spec, head_spec, head_spec, wo_spec, row_spec, row_spec, expert_spec, expert_spec, expert_spec), out_specs=row_spec, check_vma=False)
```

```python
import functools
import jax
import jax.numpy as jnp
from jax import lax
from jax.experimental import pallas as pl
from jax.experimental.pallas import tpu as pltpu
from jax.sharding import PartitionSpec as P

QB = 256
KB = 512
CH = 128
HC = 64
OVER_X = (7,)
OV = 32
LIMIT = OV
WR = 256
LOG2E = 1.4426950408889634
VLIM = 60 * 1024 * 1024
MESH = pl.DeviceIdType.MESH


def attend_block(q_of, kv_ref, m_ref, l_ref, acc_ref, pos0, heads, hd):
    c = (hd ** -0.5) * LOG2E
    m_ref[...] = jnp.full(m_ref.shape, -jnp.inf, jnp.float32)
    l_ref[...] = jnp.zeros(l_ref.shape, jnp.float32)
    acc_ref[...] = jnp.zeros(acc_ref.shape, jnp.float32)

    def step(kb, masked):
        start = pl.multiple_of(kb * KB, KB)
        k = kv_ref[pl.ds(start, KB), :hd]
        v = kv_ref[pl.ds(start, KB), hd:]
        score = lambda h: lax.dot_general(q_of(h), k, (((1,), (1,)), ((), ())), preferred_element_type=jnp.float32)
        if masked:
            qp = pos0 + lax.broadcasted_iota(jnp.int32, (QB, KB), 0)
            kp = start + lax.broadcasted_iota(jnp.int32, (QB, KB), 1)
            keep = kp <= qp
        s_next = score(0)
        for h in range(heads):
            rows = slice(h * QB, (h + 1) * QB)
            s = s_next
            if h + 1 < heads:
                s_next = score(h + 1)
            if masked:
                s = jnp.where(keep, s, -jnp.inf)
            m_old = m_ref[rows, :]
            m_new = jnp.maximum(m_old, jnp.max(s, axis=1, keepdims=True))
            alpha = jnp.exp2((m_old - m_new) * c)
            p = jnp.exp2((s - jnp.concatenate([m_new] * (KB // 128), axis=1)) * c)
            lp = p[:, :128]
            for j in range(1, KB // 128):
                lp = lp + p[:, j * 128:(j + 1) * 128]
            m_ref[rows, :] = m_new
            l_ref[rows, :] = l_ref[rows, :] * alpha + lp
            acc_ref[rows, :] = acc_ref[rows, :] * alpha + jnp.dot(p.astype(jnp.bfloat16), v, preferred_element_type=jnp.float32)

    last = pos0 // KB

    def body(kb, carry):
        step(kb, False)
        return carry

    lax.fori_loop(0, last, body, 0)
    step(last, True)


def rdma(src, dst, send_sem, recv_sem, cp, tp):
    return pltpu.make_async_remote_copy(src_ref=src, dst_ref=dst, send_sem=send_sem, recv_sem=recv_sem, device_id=(0, cp, tp), device_id_type=MESH)


def await_bytes(ref, sem):
    pltpu.make_async_copy(ref, ref, sem).wait()


def greet(others):
    barrier = pltpu.get_barrier_semaphore()
    for cp, tp in others:
        pl.semaphore_signal(barrier, inc=1, device_id=(0, cp, tp), device_id_type=MESH)
    pl.semaphore_wait(barrier, len(others))


def slot_rows(idx_ref, num_exp, exp_local, cap):
    rows = idx_ref.shape[1]
    expert = lax.broadcasted_iota(jnp.int32, (num_exp, rows), 0)
    hot = [jnp.where(idx_ref[k:k + 1, :] == expert, 1.0, 0.0) for k in range(2)]
    earlier = lax.broadcasted_iota(jnp.int32, (rows, rows), 0) < lax.broadcasted_iota(jnp.int32, (rows, rows), 1)
    earlier = jnp.where(earlier, 1.0, 0.0).astype(jnp.bfloat16)
    count = jnp.dot((hot[0] + hot[1]).astype(jnp.bfloat16), earlier, preferred_element_type=jnp.float32)
    lane_sum = jnp.sum(hot[0] + hot[1], axis=1, keepdims=True)
    over = jnp.maximum(lane_sum - cap // 2, 0.0)
    e0 = lax.broadcasted_iota(jnp.int32, (num_exp, num_exp), 0)
    e1 = lax.broadcasted_iota(jnp.int32, (num_exp, num_exp), 1)
    before = jnp.where(jnp.logical_and(e0 // exp_local == e1 // exp_local, e1 < e0), 1.0, 0.0).astype(jnp.bfloat16)
    offset = jnp.dot(before, jnp.broadcast_to(over, (num_exp, num_exp)).astype(jnp.bfloat16), preferred_element_type=jnp.float32)[:, 0:1]
    worst = jnp.broadcast_to(jnp.max(offset + over, axis=0, keepdims=True), (1, rows)).astype(jnp.int32)
    slots, ranks = [], []
    for k in range(2):
        pos = jnp.sum(hot[k] * count, axis=0, keepdims=True)
        rank = jnp.sum(hot[k] * offset, axis=0, keepdims=True) + pos - cap // 2
        slots.append(idx_ref[k:k + 1, :] * cap + pos.astype(jnp.int32))
        ranks.append(jnp.where(pos >= cap // 2, rank, -1.0).astype(jnp.int32))
    return slots + ranks + [worst]


def front_kernel(cp_size, tp_size, heads, hd, num_exp, cap, x_ref, idx_ref, wq_ref, wk_ref, wv_ref, wo_ref, h_ref, tok_ref, hbuf, own_slots, slots,
                 x_all, wq, wkv, wo, q_ref, kv_ref, m_ref, l_ref, acc_ref, ob_ref, part, from_near, from_far,
                 wsem, slot_send, slot_recv, x_send, x_near, x_far, x_fwd_send, x_fwd, kv_send, kv_recv,
                 near_send, near_recv, far_send, far_recv, h_send, h_near, h_far, h_peer, h_diag, load_sem, tok_sem, raw, raw_sem):
    r, t = lax.axis_index('cp'), lax.axis_index('tp')
    num_devs = cp_size * tp_size
    me = r * tp_size + t
    near = t + 1 - 2 * lax.rem(t, 2)
    far = lax.rem(t + 2, tp_size)
    far_near = lax.rem(near + 2, tp_size)
    peer = 1 - r
    rows, width = x_ref.shape
    half_rows = rows // 2
    devs = [lax.rem(me + j, num_devs) for j in range(1, num_devs)]

    weights = [pltpu.make_async_copy(wk_ref, wkv.at[:, pl.ds(0, hd)], wsem.at[0]), pltpu.make_async_copy(wv_ref, wkv.at[:, pl.ds(hd, hd)], wsem.at[1]), pltpu.make_async_copy(wo_ref, wo, wsem.at[2])]
    for copy in weights:
        copy.start()

    def raw_copy(k, slot):
        return pltpu.make_async_copy(wq_ref.at[pl.ds(pl.multiple_of(k * WR, WR), WR)], raw.at[slot], raw_sem.at[slot])

    for k in range(2):
        raw_copy(k, k).start()
    greet([(d // tp_size, lax.rem(d, tp_size)) for d in devs])
    chunks = rows // CH
    for j in range(chunks):
        at = pl.ds(j * CH, CH)
        rdma(x_ref.at[at], x_all.at[0, at], x_send, x_far.at[j], r, far).start()
    rdma(x_ref, x_all.at[1], x_send, x_near, r, near).start()
    mine = slot_rows(idx_ref, num_exp, num_exp // num_devs, cap)
    own_slots[...] = jnp.concatenate(mine + [jnp.zeros((3, rows), jnp.int32)], axis=0)
    slots[me] = own_slots[...]
    for d in devs:
        rdma(own_slots, slots.at[me], slot_send, slot_recv, d // tp_size, lax.rem(d, tp_size)).start()
    for copy in weights[:2]:
        copy.wait()

    def flatten(k, carry):
        slot = lax.rem(k, 2)
        raw_copy(k, slot).wait()
        at = pl.ds(pl.multiple_of(k * WR, WR), WR)
        for h in range(heads):
            wq[at, h * hd:(h + 1) * hd] = raw[slot, :, h, :]

        @pl.when(k + 2 < width // WR)
        def _():
            raw_copy(k + 2, slot).start()

        return carry

    lax.fori_loop(0, width // WR, flatten, 0)

    def project(x, tp_src, row0, count):
        half = row0 // half_rows
        seg = r + half * (2 * cp_size - 1 - 2 * r)
        pos = pl.multiple_of((seg * tp_size + tp_src) * half_rows + row0 % half_rows, CH)
        kv_ref[pl.ds(pos, count), :] = jnp.dot(x, wkv[...], preferred_element_type=jnp.float32).astype(jnp.bfloat16)
        sent = kv_ref.at[pl.ds(pos, count)]
        rdma(sent, sent, kv_send, kv_recv.at[half], peer, t).start()
        at = pl.ds(pl.multiple_of(tp_src * rows + row0, CH), count)
        q_ref[at, :] = jnp.dot(x, wq[...], preferred_element_type=jnp.float32).astype(jnp.bfloat16)

    def project_far(half):
        def chunk(j, carry):
            first = pl.multiple_of(j * CH, CH)
            at = pl.ds(first, CH)
            await_bytes(x_all.at[0, at], x_far.at[j])
            rdma(x_all.at[0, at], x_all.at[2, at], x_fwd_send, x_fwd.at[j], r, near).start()
            project(x_all[0, at, :], far, first, CH)
            await_bytes(x_all.at[2, at], x_fwd.at[j])
            project(x_all[2, at, :], far_near, first, CH)
            return carry

        lax.fori_loop(half * (chunks // 2), (half + 1) * (chunks // 2), chunk, 0)
        await_bytes(kv_ref.at[pl.ds(0, tp_size * half_rows)], kv_recv.at[half])

    def project_half(x_at, tp_src):
        def step(half, carry):
            first = pl.multiple_of(half * half_rows, half_rows)
            project(x_at[pl.ds(first, half_rows), :], tp_src, first, half_rows)
            return carry

        lax.fori_loop(0, 2, step, 0)

    project_half(x_ref, t)
    await_bytes(x_all.at[1], x_near)
    project_half(x_all.at[1], near)
    project_far(0)
    weights[2].wait()

    def h_rows(cp, tp, j):
        return h_ref.at[pl.ds(pl.multiple_of((cp * tp_size + tp) * rows + j * HC, HC), HC)]

    def h_block(cp, tp):
        return h_ref.at[pl.ds(pl.multiple_of((cp * tp_size + tp) * rows, rows), rows)]

    OWN, PEER, FAR, DIAG = range(4)
    h_chunks = rows // HC

    def finish(half):
        await_bytes(from_near.at[2 + half], near_recv.at[2 + half])
        for within in range(0, QB, HC):
            first = half * QB + within
            j = first // HC
            at = slice(within, within + HC)
            if within % CH == 0:
                await_bytes(from_far.at[half, pl.ds(within, CH)], far_recv.at[half, within // CH])
            total = part[4 + half, at, :] + from_near[2 + half, at, :] + from_far[half, at, :]
            hbuf[first:first + HC, :] = (x_ref[first:first + HC, :].astype(jnp.float32) + total).astype(jnp.bfloat16)
            src = hbuf.at[pl.ds(first, HC)]
            mine = h_rows(r, t, j)
            rdma(src, mine, h_send, h_far.at[j], r, far).start()
            rdma(src, mine, h_send, h_peer.at[j], peer, t).start()
            rdma(src, mine, h_send, h_near.at[OWN], r, near).start()

    def forward(got, kind):
        rdma(got, got, h_send, h_near.at[kind], r, near).start()

    def diag(j):
        got = h_rows(peer, far, j)
        await_bytes(got, h_diag.at[j])
        forward(got, DIAG)

    def from_peer(j):
        got = h_rows(peer, t, j)
        await_bytes(got, h_peer.at[j])
        forward(got, PEER)
        if j in OVER_X:
            rdma(got, got, h_send, h_diag.at[j], r, far).start()

    def across(j):
        got = h_rows(r, far, j)
        await_bytes(got, h_far.at[j])
        forward(got, FAR)
        if j not in OVER_X:
            rdma(got, got, h_send, h_diag.at[j], peer, t).start()

    def block(i, carry):
        half = i // 4
        local = lax.rem(i // 2, 2)
        mine = lax.rem(i, 2)
        slot = mine * (2 + 2 * local) + half

        @pl.when(i == 4)
        def _():
            project_far(1)

        @pl.when(i == 5)
        def _():
            finish(0)

        @pl.when(i == 7)
        def _():
            for j in range(h_chunks // 2):
                from_peer(j)
            for j in range(h_chunks // 2):
                across(j)

        @pl.when(jnp.logical_and(mine == 0, local == 1))
        def _():
            await_bytes(part.at[half], near_send.at[half])

        t_dst = lax.rem(mine * t + (1 - mine) * near + 2 * (1 - local), tp_size)
        seg = r + half * (2 * cp_size - 1 - 2 * r)
        pos0 = (seg * tp_size + t_dst) * QB
        row0 = pl.multiple_of(t_dst * rows + half * QB, QB)
        attend_block(lambda h: q_ref[pl.ds(row0, QB), h * hd:(h + 1) * hd], kv_ref, m_ref, l_ref, acc_ref, pos0, heads, hd)
        for h in range(heads):
            at = slice(h * QB, (h + 1) * QB)
            den = jnp.sum(l_ref[at, :], axis=1, keepdims=True)
            ob_ref[:, h * hd:(h + 1) * hd] = (acc_ref[at, :] / den).astype(jnp.bfloat16)
        part[slot] = jnp.dot(ob_ref[...], wo[...], preferred_element_type=jnp.float32)

        @pl.when(mine == 0)
        def _():
            rdma(part.at[slot], from_near.at[2 * local + half], near_send.at[half], near_recv.at[2 * local + half], r, near).start()

        @pl.when(jnp.logical_and(mine == 1, local == 0))
        def _():
            await_bytes(from_near.at[half], near_recv.at[half])
            part[slot] += from_near[half]
            for c in range(QB // CH):
                at = pl.ds(c * CH, CH)
                rdma(part.at[slot, at], from_far.at[half, at], far_send, far_recv.at[half, c], r, far).start()

        return carry

    lax.fori_loop(0, 8, block, 0)
    await_bytes(x_all.at[0], x_fwd_send)

    finish(1)
    await_bytes(slots.at[pl.ds(0, num_devs - 1)], slot_recv)
    local_slots = (num_exp // num_devs) * cap

    def pick(pair, ends):
        exp_local = num_exp // num_devs
        sels = []
        for dev, _ in ends:
            ids = slots[dev] - me * local_slots
            want = lax.broadcasted_iota(jnp.int32, (local_slots, rows), 0)
            sel = jnp.logical_or(ids[0:1, :] == want, ids[1:2, :] == want)
            sels.append(jnp.where(sel, 1.0, 0.0).astype(jnp.bfloat16))
        if pair > 0:
            await_bytes(x_all.at[2], tok_sem)
        for c0 in range(0, width, 512):
            parts = [jnp.dot(sel, src[:, c0:c0 + 512], preferred_element_type=jnp.float32).reshape(exp_local, 2, cap // 2, 512) for sel, (_, src) in zip(sels, ends)]
            x_all[2, :, c0:c0 + 512] = jnp.concatenate(parts, axis=2).reshape(rows, 512).astype(jnp.bfloat16)
        for e in range(exp_local):
            for upper in range(2):
                pltpu.make_async_copy(x_all.at[2, pl.ds((2 * e + upper) * cap, cap)], tok_ref.at[e, pl.ds(upper * (num_devs * cap // 2) + pair * cap, cap)], tok_sem).start()

    def fetch(n, cp, tp):
        return pltpu.make_async_copy(h_block(cp, tp), x_all.at[n % 2], load_sem.at[n % 2])

    for j in range(h_chunks // 2):
        diag(j)
    from_peer(4)
    across(4)
    await_bytes(h_block(r, near), h_near.at[OWN])
    fetch(1, r, near).start()
    fetch(1, r, near).wait()
    pick(0, ((me, hbuf), (r * tp_size + near, x_all.at[1])))
    for j in range(5, h_chunks):
        from_peer(j)
        across(j)
    fetch(0, peer, t).start()
    await_bytes(h_block(peer, near), h_near.at[PEER])
    fetch(1, peer, near).start()
    fetch(0, peer, t).wait()
    fetch(1, peer, near).wait()
    pick(1, ((peer * tp_size + t, x_all.at[0]), (peer * tp_size + near, x_all.at[1])))
    fetch(0, r, far).start()
    await_bytes(h_block(r, far_near), h_near.at[FAR])
    fetch(1, r, far_near).start()
    fetch(0, r, far).wait()
    fetch(1, r, far_near).wait()
    pick(2, ((r * tp_size + far, x_all.at[0]), (r * tp_size + far_near, x_all.at[1])))
    for j in range(4, h_chunks):
        diag(j)
    fetch(0, peer, far).start()
    await_bytes(h_block(peer, far_near), h_near.at[DIAG])
    fetch(1, peer, far_near).start()
    fetch(0, peer, far).wait()
    fetch(1, peer, far_near).wait()
    pick(3, ((peer * tp_size + far, x_all.at[0]), (peer * tp_size + far_near, x_all.at[1])))

    await_bytes(x_all.at[2], tok_sem)
    for n in range(2):
        await_bytes(part.at[n], near_send.at[n])
    await_bytes(h_ref.at[pl.ds(0, 7 * rows)], h_send)
    await_bytes(part.at[pl.ds(0, 2)], far_send)
    await_bytes(slots.at[pl.ds(0, num_devs - 1)], slot_send)
    await_bytes(x_all.at[pl.ds(0, 2)], x_send)
    await_bytes(kv_ref.at[pl.ds(0, tp_size * rows)], kv_send)


def moe_kernel(num_devs, tp_size, exp_local, cap, full, tok_ref, h_ref, slot_ref, slots_ref, gate_ref, wg_ref, wu_ref, wd_ref, y_ref, tok, wgb, wub, wdb, zrecv, over, yacc, cols, tsem, wsem, send_sem, over_sem, recv_sem):
    rows, width = y_ref.shape
    r, t = lax.axis_index('cp'), lax.axis_index('tp')
    me = r * tp_size + t
    near = t + 1 - 2 * lax.rem(t, 2)
    places = [(cp, lax.rem(tp + 2 * across, tp_size)) for across in range(2) for cp in (r, 1 - r) for tp in (t, near)]
    low = cap // 2
    pairs = exp_local // 2
    block = num_devs * cap
    half_block = block // 2

    def weight_copies(e, slot):
        return [pltpu.make_async_copy(src.at[e], dst.at[slot], wsem.at[i, slot]) for i, (src, dst) in enumerate(((wg_ref, wgb), (wu_ref, wub), (wd_ref, wdb)))]

    loads = [pltpu.make_async_copy(tok_ref.at[at], tok.at[at], tsem.at[n]) for n, at in enumerate((pl.ds(0, 2), pl.ds(2, exp_local - 2)))]
    for e in range(2):
        loads[e].start()
        for copy in weight_copies(e, e):
            copy.start()
    greet(places[1:])
    slot = slot_ref[0:2, :]
    pos = slot % cap
    expert = slot // cap
    dev = expert // exp_local
    el = expert % exp_local
    dev_cp, dev_tp = dev // tp_size, dev % tp_size
    place = jnp.where(dev_tp % 2 == t % 2, 0, 1) + jnp.where(dev_cp == r, 0, 2) + jnp.where(dev_tp // 2 == t // 2, 0, 4)
    home = (el // 2) * block + place * cap + (el % 2) * low + pos % low
    upper = pairs * block + (home if full else place * OV + slot_ref[2:4, :])
    back = jnp.where(pos < low, home, upper)
    columns = jnp.concatenate([back.astype(jnp.float32), gate_ref[...], jnp.zeros((124, rows), jnp.float32)], axis=0)
    cols[...] = jnp.transpose(columns)
    yacc[...] = h_ref[...].astype(jnp.float32)
    loads[0].wait()

    def send(src, dst, sem, group, n):
        rdma(src, dst, sem, recv_sem.at[group], *places[n]).start()

    def two_experts(m, carry):
        @pl.when(m == 1)
        def _():
            loads[1].wait()

        outs = []
        for b in range(2):
            e = 2 * m + b
            for copy in weight_copies(e, b):
                copy.wait()
            x = tok[e]
            gate = jnp.dot(x, wgb[b], preferred_element_type=jnp.float32)
            up = jnp.dot(x, wub[b], preferred_element_type=jnp.float32)
            act = (jax.nn.silu(gate) * up).astype(jnp.bfloat16)
            outs.append(jnp.dot(act, wdb[b], preferred_element_type=jnp.float32))

            @pl.when(e + 2 < exp_local)
            def _():
                for copy in weight_copies(e + 2, b):
                    copy.start()

        for side in range(2):
            pieces = [z[side * half_block:(side + 1) * half_block].reshape(num_devs, low, width) for z in outs]
            tok[2 * m + side] = jnp.concatenate(pieces, axis=1).reshape(block, width).astype(jnp.bfloat16)
            if side == 0 or full:
                at = side * pairs + m
                for n in range(1, num_devs):
                    part = pl.ds(n * cap, cap)
                    send(tok.at[2 * m + side, part], zrecv.at[at, part], over_sem if side else send_sem, at // 2, n)
                zrecv[at, :cap, :] = tok[2 * m + side, :cap, :]
        return carry

    lax.fori_loop(0, pairs, two_experts, 0)

    if not full:
        per_block = block // OV
        for n in (4, 5, 6, 7, 2, 3, 1, 0):
            cp, tp = places[n]
            ids = slots_ref[cp * tp_size + tp]
            mix = jnp.zeros((OV, half_block), jnp.float32)
            for k in range(2):
                own = ids[k:k + 1, :] - me * exp_local * cap
                inside = jnp.logical_and(own >= 0, own < exp_local * cap)
                spot = jnp.where(jnp.logical_and(inside, own % cap >= low), own // cap * low + own % cap - low, -1)
                a = jnp.where(ids[2 + k:3 + k, :] == lax.broadcasted_iota(jnp.int32, (OV, rows), 0), 1.0, 0.0).astype(jnp.bfloat16)
                b = jnp.where(spot == lax.broadcasted_iota(jnp.int32, (half_block * 2, rows), 0), 1.0, 0.0).astype(jnp.bfloat16)
                mix = lax.dot_general(a, b, (((1,), (1,)), ((), ())), preferred_element_type=jnp.float32) + (mix if k else 0.0)
            mix = mix.astype(jnp.bfloat16)
            for c0 in range(0, width, 512):
                z = jnp.concatenate([tok[2 * m + 1, n * cap:(n + 1) * cap, c0:c0 + 512] for m in range(pairs)], axis=0)
                over[n, :, c0:c0 + 512] = jnp.dot(mix, z, preferred_element_type=jnp.float32).astype(jnp.bfloat16)
            dst = zrecv.at[pairs + n // per_block, pl.ds(n % per_block * OV, OV)]
            if n:
                send(over.at[n], dst, over_sem, pairs // 2, n)
            else:
                dst[...] = over[n]

    groups = recv_sem.shape[0]
    span = 2 * block

    def combine(g, carry):
        await_bytes(zrecv.at[pl.ds(0, 2), pl.ds(0, (num_devs - 1) * cap)], recv_sem.at[g])
        want = (lax.broadcasted_iota(jnp.int32, (rows, span), 1) + g * span).astype(jnp.float32)
        sel0 = jnp.where(cols[:, 0:1] == want, 1.0, 0.0).astype(jnp.bfloat16)
        sel1 = jnp.where(cols[:, 1:2] == want, 1.0, 0.0).astype(jnp.bfloat16)
        first = pl.multiple_of(g * 2, 2)
        for c0 in range(0, width, 512):
            z = zrecv[pl.ds(first, 2), :, c0:c0 + 512].reshape(span, 512)
            z0 = jnp.dot(sel0, z, preferred_element_type=jnp.float32)
            z1 = jnp.dot(sel1, z, preferred_element_type=jnp.float32)
            yacc[:, c0:c0 + 512] += cols[:, 2:3] * z0 + cols[:, 3:4] * z1
        return carry

    lax.fori_loop(0, groups, combine, 0)
    y_ref[...] = yacc[...].astype(y_ref.dtype)
    await_bytes(tok.at[pl.ds(0, pairs), pl.ds(0, (num_devs - 1) * cap)], send_sem)
    await_bytes(tok.at[pl.ds(0, pairs if full else 2), pl.ds(0, (num_devs - 1) * cap)], over_sem)


def solution(mesh):
    cp_size = mesh.shape['cp']
    tp_size = mesh.shape['tp']
    num_devs = cp_size * tp_size
    row_spec = P(('data', 'cp', 'tp'), None)
    head_spec = P(None, 'tp', None)
    wo_spec = P('tp', None, None)
    expert_spec = P(('cp', 'tp'), None, None)

    vmem = pl.BlockSpec(memory_space=pltpu.VMEM)
    hbm = pl.BlockSpec(memory_space=pl.ANY)
    dma = pltpu.SemaphoreType.DMA
    bf16, f32 = jnp.bfloat16, jnp.float32

    def params(number):
        return pltpu.CompilerParams(collective_id=number, has_side_effects=True, vmem_limit_bytes=VLIM)

    def front(x_blk, idx, w_q, w_k, w_v, w_o, heads, hd, exp_local, cap):
        rows, width = x_blk.shape
        group = rows * tp_size
        v32 = lambda *shape: pltpu.VMEM(shape, f32)
        v16 = lambda *shape: pltpu.VMEM(shape, bf16)
        return pl.pallas_call(
            functools.partial(front_kernel, cp_size, tp_size, heads, hd, exp_local * num_devs, cap),
            in_specs=[vmem, vmem, hbm, hbm, hbm, hbm],
            out_specs=[hbm, hbm, vmem, vmem, vmem],
            out_shape=[jax.ShapeDtypeStruct((rows * num_devs, width), bf16), jax.ShapeDtypeStruct((exp_local, num_devs * cap, width), bf16), jax.ShapeDtypeStruct((rows, width), bf16), jax.ShapeDtypeStruct((8, rows), jnp.int32), jax.ShapeDtypeStruct((num_devs, 8, rows), jnp.int32)],
            scratch_shapes=[
                v16(3, rows, width), v16(width, heads * hd), v16(width, 2 * hd), v16(heads * hd, width), v16(group, heads * hd), v16(group * cp_size, 2 * hd),
                v32(heads * QB, 128), v32(heads * QB, 128), v32(heads * QB, hd), v16(QB, heads * hd),
                v32(6, QB, width), v32(4, QB, width), v32(2, QB, width),
                dma((3,)), dma, dma, dma, dma, dma((rows // CH,)), dma, dma((rows // CH,)), dma, dma((2,)),
                dma((2,)), dma((4,)), dma, dma((2, QB // CH)), dma, dma((4,)), dma((rows // HC,)), dma((rows // HC,)), dma((rows // HC,)), dma((2,)), dma, v16(2, WR, heads, hd), dma((2,))],
            compiler_params=params(0),
            name='front',
        )(x_blk, idx, w_q, w_k, w_v, w_o)

    def experts(full, cap, tok, h_own, own_slots, slots, gates, w_gate, w_up, w_down):
        rows, width = h_own.shape
        exp_local, _, ff = w_gate.shape
        v16 = lambda *shape: pltpu.VMEM(shape, bf16)
        block = num_devs * cap
        blocks = exp_local if full else exp_local // 2 + num_devs * OV // block
        return pl.pallas_call(
            functools.partial(moe_kernel, num_devs, tp_size, exp_local, cap, full),
            in_specs=[hbm, vmem, vmem, vmem, vmem, hbm, hbm, hbm],
            out_specs=vmem,
            out_shape=jax.ShapeDtypeStruct((rows, width), bf16),
            scratch_shapes=[v16(exp_local, block, width), v16(2, width, ff), v16(2, width, ff), v16(2, ff, width), v16(blocks, block, width), v16(num_devs, OV, width), pltpu.VMEM((rows, width), f32), pltpu.VMEM((rows, 128), f32), dma((2,)), dma((3, 2)), dma, dma, dma((blocks // 2,))],
            compiler_params=params(2 if full else 1),
            name='moe_full' if full else 'moe',
        )(tok, h_own, own_slots, slots, gates, w_gate, w_up, w_down)

    def device_fn(x_blk, w_q, w_k, w_v, w_o, idx_blk, gate_blk, w_gate, w_up, w_down):
        tok_dev, width = x_blk.shape
        heads, head_dim = w_q.shape[1], w_k.shape[2]
        exp_local = w_gate.shape[0]
        num_exp = exp_local * num_devs
        capacity = 4 * tok_dev // num_exp

        flat = lambda w: w.reshape(width, -1)
        _, tok, h_own, own_slots, slots = front(x_blk, idx_blk.T, w_q, flat(w_k), flat(w_v), w_o.reshape(heads * head_dim, width), heads, head_dim, exp_local, capacity)
        few = jnp.max(slots[:, 4, 0]) <= LIMIT
        return lax.cond(few, functools.partial(experts, False, capacity), functools.partial(experts, True, capacity), tok, h_own, own_slots, slots, gate_blk.T, w_gate, w_up, w_down)

    return jax.shard_map(device_fn, mesh=mesh, in_specs=(row_spec, head_spec, head_spec, head_spec, wo_spec, row_spec, row_spec, expert_spec, expert_spec, expert_spec), out_specs=row_spec, check_vma=False)
```

```python
import functools
import jax
import jax.numpy as jnp
from jax import lax
from jax.experimental import pallas as pl
from jax.experimental.pallas import tpu as pltpu
from jax.sharding import PartitionSpec as P

QB = 256
KB = 512
CH = 128
HC = 64
OVER_X = (7,)
OV = 32
LIMIT = OV
WR = 256
LOG2E = 1.4426950408889634
VLIM = 60 * 1024 * 1024
MESH = pl.DeviceIdType.MESH


def attend_block(q_of, kv_ref, m_ref, l_ref, acc_ref, pos0, heads, hd):
    c = (hd ** -0.5) * LOG2E
    m_ref[...] = jnp.full(m_ref.shape, -jnp.inf, jnp.float32)
    l_ref[...] = jnp.zeros(l_ref.shape, jnp.float32)
    acc_ref[...] = jnp.zeros(acc_ref.shape, jnp.float32)

    def step(kb, masked):
        start = pl.multiple_of(kb * KB, KB)
        k = kv_ref[pl.ds(start, KB), :hd]
        v = kv_ref[pl.ds(start, KB), hd:]
        score = lambda h: lax.dot_general(q_of(h), k, (((1,), (1,)), ((), ())), preferred_element_type=jnp.float32)
        if masked:
            qp = pos0 + lax.broadcasted_iota(jnp.int32, (QB, KB), 0)
            kp = start + lax.broadcasted_iota(jnp.int32, (QB, KB), 1)
            keep = kp <= qp
        s_next = score(0)
        for h in range(heads):
            rows = slice(h * QB, (h + 1) * QB)
            s = s_next
            if h + 1 < heads:
                s_next = score(h + 1)
            if masked:
                s = jnp.where(keep, s, -jnp.inf)
            m_old = m_ref[rows, :]
            m_new = jnp.maximum(m_old, jnp.max(s, axis=1, keepdims=True))
            alpha = jnp.exp2((m_old - m_new) * c)
            p = jnp.exp2((s - jnp.concatenate([m_new] * (KB // 128), axis=1)) * c)
            lp = p[:, :128]
            for j in range(1, KB // 128):
                lp = lp + p[:, j * 128:(j + 1) * 128]
            m_ref[rows, :] = m_new
            l_ref[rows, :] = l_ref[rows, :] * alpha + lp
            acc_ref[rows, :] = acc_ref[rows, :] * alpha + jnp.dot(p.astype(jnp.bfloat16), v, preferred_element_type=jnp.float32)

    last = pos0 // KB

    def body(kb, carry):
        step(kb, False)
        return carry

    lax.fori_loop(0, last, body, 0)
    step(last, True)


def rdma(src, dst, send_sem, recv_sem, cp, tp):
    return pltpu.make_async_remote_copy(src_ref=src, dst_ref=dst, send_sem=send_sem, recv_sem=recv_sem, device_id=(0, cp, tp), device_id_type=MESH)


def await_bytes(ref, sem):
    pltpu.make_async_copy(ref, ref, sem).wait()


def greet(others):
    barrier = pltpu.get_barrier_semaphore()
    for cp, tp in others:
        pl.semaphore_signal(barrier, inc=1, device_id=(0, cp, tp), device_id_type=MESH)
    pl.semaphore_wait(barrier, len(others))


def slot_rows(idx_ref, num_exp, exp_local, cap):
    rows = idx_ref.shape[1]
    expert = lax.broadcasted_iota(jnp.int32, (num_exp, rows), 0)
    hot = [jnp.where(idx_ref[k:k + 1, :] == expert, 1.0, 0.0) for k in range(2)]
    earlier = lax.broadcasted_iota(jnp.int32, (rows, rows), 0) < lax.broadcasted_iota(jnp.int32, (rows, rows), 1)
    earlier = jnp.where(earlier, 1.0, 0.0).astype(jnp.bfloat16)
    count = jnp.dot((hot[0] + hot[1]).astype(jnp.bfloat16), earlier, preferred_element_type=jnp.float32)
    lane_sum = jnp.sum(hot[0] + hot[1], axis=1, keepdims=True)
    over = jnp.maximum(lane_sum - cap // 2, 0.0)
    e0 = lax.broadcasted_iota(jnp.int32, (num_exp, num_exp), 0)
    e1 = lax.broadcasted_iota(jnp.int32, (num_exp, num_exp), 1)
    before = jnp.where(jnp.logical_and(e0 // exp_local == e1 // exp_local, e1 < e0), 1.0, 0.0).astype(jnp.bfloat16)
    offset = jnp.dot(before, jnp.broadcast_to(over, (num_exp, num_exp)).astype(jnp.bfloat16), preferred_element_type=jnp.float32)[:, 0:1]
    worst = jnp.broadcast_to(jnp.max(offset + over, axis=0, keepdims=True), (1, rows)).astype(jnp.int32)
    slots, ranks = [], []
    for k in range(2):
        pos = jnp.sum(hot[k] * count, axis=0, keepdims=True)
        rank = jnp.sum(hot[k] * offset, axis=0, keepdims=True) + pos - cap // 2
        slots.append(idx_ref[k:k + 1, :] * cap + pos.astype(jnp.int32))
        ranks.append(jnp.where(pos >= cap // 2, rank, -1.0).astype(jnp.int32))
    return slots + ranks + [worst]


def front_kernel(cp_size, tp_size, heads, hd, num_exp, cap, x_ref, idx_ref, wq_ref, wk_ref, wv_ref, wo_ref, h_ref, tok_ref, hbuf, own_slots, slots,
                 x_all, wq, wkv, wo, q_ref, kv_ref, m_ref, l_ref, acc_ref, ob_ref, part, from_near, from_far,
                 wsem, slot_send, slot_recv, x_send, x_near, x_far, x_fwd_send, x_fwd, kv_send, kv_recv,
                 near_send, near_recv, far_send, far_recv, h_send, h_near, h_far, h_peer, h_diag, load_sem, tok_sem, raw, raw_sem):
    r, t = lax.axis_index('cp'), lax.axis_index('tp')
    num_devs = cp_size * tp_size
    me = r * tp_size + t
    near = t + 1 - 2 * lax.rem(t, 2)
    far = lax.rem(t + 2, tp_size)
    far_near = lax.rem(near + 2, tp_size)
    peer = 1 - r
    rows, width = x_ref.shape
    half_rows = rows // 2
    devs = [lax.rem(me + j, num_devs) for j in range(1, num_devs)]

    weights = [pltpu.make_async_copy(wk_ref, wkv.at[:, pl.ds(0, hd)], wsem.at[0]), pltpu.make_async_copy(wv_ref, wkv.at[:, pl.ds(hd, hd)], wsem.at[1]), pltpu.make_async_copy(wo_ref, wo, wsem.at[2])]
    for copy in weights:
        copy.start()

    def raw_copy(k, slot):
        return pltpu.make_async_copy(wq_ref.at[pl.ds(pl.multiple_of(k * WR, WR), WR)], raw.at[slot], raw_sem.at[slot])

    for k in range(2):
        raw_copy(k, k).start()
    greet([(d // tp_size, lax.rem(d, tp_size)) for d in devs])
    chunks = rows // CH
    for j in range(chunks):
        at = pl.ds(j * CH, CH)
        rdma(x_ref.at[at], x_all.at[0, at], x_send, x_far.at[j], r, far).start()
    rdma(x_ref, x_all.at[1], x_send, x_near, r, near).start()
    mine = slot_rows(idx_ref, num_exp, num_exp // num_devs, cap)
    own_slots[...] = jnp.concatenate(mine + [jnp.zeros((3, rows), jnp.int32)], axis=0)
    slots[me] = own_slots[...]
    for d in devs:
        rdma(own_slots, slots.at[me], slot_send, slot_recv, d // tp_size, lax.rem(d, tp_size)).start()
    for copy in weights[:2]:
        copy.wait()

    def flatten(k, carry):
        slot = lax.rem(k, 2)
        raw_copy(k, slot).wait()
        at = pl.ds(pl.multiple_of(k * WR, WR), WR)
        for h in range(heads):
            wq[at, h * hd:(h + 1) * hd] = raw[slot, :, h, :]

        @pl.when(k + 2 < width // WR)
        def _():
            raw_copy(k + 2, slot).start()

        return carry

    lax.fori_loop(0, width // WR, flatten, 0)

    def project(x, tp_src, row0, count):
        half = row0 // half_rows
        seg = r + half * (2 * cp_size - 1 - 2 * r)
        pos = pl.multiple_of((seg * tp_size + tp_src) * half_rows + row0 % half_rows, CH)
        kv_ref[pl.ds(pos, count), :] = jnp.dot(x, wkv[...], preferred_element_type=jnp.float32).astype(jnp.bfloat16)
        sent = kv_ref.at[pl.ds(pos, count)]
        rdma(sent, sent, kv_send, kv_recv.at[half], peer, t).start()
        at = pl.ds(pl.multiple_of(tp_src * rows + row0, CH), count)
        q_ref[at, :] = jnp.dot(x, wq[...], preferred_element_type=jnp.float32).astype(jnp.bfloat16)

    def project_far(half):
        def chunk(j, carry):
            first = pl.multiple_of(j * CH, CH)
            at = pl.ds(first, CH)
            await_bytes(x_all.at[0, at], x_far.at[j])
            rdma(x_all.at[0, at], x_all.at[2, at], x_fwd_send, x_fwd.at[j], r, near).start()
            project(x_all[0, at, :], far, first, CH)
            await_bytes(x_all.at[2, at], x_fwd.at[j])
            project(x_all[2, at, :], far_near, first, CH)
            return carry

        lax.fori_loop(half * (chunks // 2), (half + 1) * (chunks // 2), chunk, 0)
        await_bytes(kv_ref.at[pl.ds(0, tp_size * half_rows)], kv_recv.at[half])

    def project_half(x_at, tp_src):
        def step(half, carry):
            first = pl.multiple_of(half * half_rows, half_rows)
            project(x_at[pl.ds(first, half_rows), :], tp_src, first, half_rows)
            return carry

        lax.fori_loop(0, 2, step, 0)

    project_half(x_ref, t)
    await_bytes(x_all.at[1], x_near)
    project_half(x_all.at[1], near)
    project_far(0)
    weights[2].wait()

    def h_rows(cp, tp, j):
        return h_ref.at[pl.ds(pl.multiple_of((cp * tp_size + tp) * rows + j * HC, HC), HC)]

    def h_block(cp, tp):
        return h_ref.at[pl.ds(pl.multiple_of((cp * tp_size + tp) * rows, rows), rows)]

    OWN, PEER, FAR, DIAG = range(4)
    h_chunks = rows // HC

    def finish(half):
        await_bytes(from_near.at[2 + half], near_recv.at[2 + half])
        for within in range(0, QB, HC):
            first = half * QB + within
            j = first // HC
            at = slice(within, within + HC)
            if within % CH == 0:
                await_bytes(from_far.at[half, pl.ds(within, CH)], far_recv.at[half, within // CH])
            total = part[4 + half, at, :] + from_near[2 + half, at, :] + from_far[half, at, :]
            hbuf[first:first + HC, :] = (x_ref[first:first + HC, :].astype(jnp.float32) + total).astype(jnp.bfloat16)
            src = hbuf.at[pl.ds(first, HC)]
            mine = h_rows(r, t, j)
            rdma(src, mine, h_send, h_far.at[j], r, far).start()
            rdma(src, mine, h_send, h_peer.at[j], peer, t).start()
            rdma(src, mine, h_send, h_near.at[OWN], r, near).start()

    def forward(got, kind):
        rdma(got, got, h_send, h_near.at[kind], r, near).start()

    def diag(j):
        got = h_rows(peer, far, j)
        await_bytes(got, h_diag.at[j])
        forward(got, DIAG)

    def from_peer(j):
        got = h_rows(peer, t, j)
        await_bytes(got, h_peer.at[j])
        forward(got, PEER)
        if j in OVER_X:
            rdma(got, got, h_send, h_diag.at[j], r, far).start()

    def across(j):
        got = h_rows(r, far, j)
        await_bytes(got, h_far.at[j])
        forward(got, FAR)
        if j not in OVER_X:
            rdma(got, got, h_send, h_diag.at[j], peer, t).start()

    def block(i, carry):
        half = i // 4
        local = lax.rem(i // 2, 2)
        mine = lax.rem(i, 2)
        slot = mine * (2 + 2 * local) + half

        @pl.when(i == 4)
        def _():
            project_far(1)

        @pl.when(i == 5)
        def _():
            finish(0)

        @pl.when(i == 7)
        def _():
            for j in range(h_chunks // 2):
                from_peer(j)
            for j in range(h_chunks // 2):
                across(j)

        @pl.when(jnp.logical_and(mine == 0, local == 1))
        def _():
            await_bytes(part.at[half], near_send.at[half])

        t_dst = lax.rem(mine * t + (1 - mine) * near + 2 * (1 - local), tp_size)
        seg = r + half * (2 * cp_size - 1 - 2 * r)
        pos0 = (seg * tp_size + t_dst) * QB
        row0 = pl.multiple_of(t_dst * rows + half * QB, QB)
        attend_block(lambda h: q_ref[pl.ds(row0, QB), h * hd:(h + 1) * hd], kv_ref, m_ref, l_ref, acc_ref, pos0, heads, hd)
        for h in range(heads):
            at = slice(h * QB, (h + 1) * QB)
            den = jnp.sum(l_ref[at, :], axis=1, keepdims=True)
            ob_ref[:, h * hd:(h + 1) * hd] = (acc_ref[at, :] / den).astype(jnp.bfloat16)
        part[slot] = jnp.dot(ob_ref[...], wo[...], preferred_element_type=jnp.float32)

        @pl.when(mine == 0)
        def _():
            rdma(part.at[slot], from_near.at[2 * local + half], near_send.at[half], near_recv.at[2 * local + half], r, near).start()

        @pl.when(jnp.logical_and(mine == 1, local == 0))
        def _():
            await_bytes(from_near.at[half], near_recv.at[half])
            part[slot] += from_near[half]
            for c in range(QB // CH):
                at = pl.ds(c * CH, CH)
                rdma(part.at[slot, at], from_far.at[half, at], far_send, far_recv.at[half, c], r, far).start()

        return carry

    lax.fori_loop(0, 8, block, 0)
    await_bytes(x_all.at[0], x_fwd_send)

    finish(1)
    await_bytes(slots.at[pl.ds(0, num_devs - 1)], slot_recv)
    local_slots = (num_exp // num_devs) * cap

    def pick(pair, ends):
        exp_local = num_exp // num_devs
        sels = []
        for dev, _ in ends:
            ids = slots[dev] - me * local_slots
            want = lax.broadcasted_iota(jnp.int32, (local_slots, rows), 0)
            sel = jnp.logical_or(ids[0:1, :] == want, ids[1:2, :] == want)
            sels.append(jnp.where(sel, 1.0, 0.0).astype(jnp.bfloat16))
        if pair > 0:
            await_bytes(x_all.at[2], tok_sem)
        for c0 in range(0, width, 512):
            parts = [jnp.dot(sel, src[:, c0:c0 + 512], preferred_element_type=jnp.float32).reshape(exp_local, 2, cap // 2, 512) for sel, (_, src) in zip(sels, ends)]
            x_all[2, :, c0:c0 + 512] = jnp.concatenate(parts, axis=2).reshape(rows, 512).astype(jnp.bfloat16)
        for e in range(exp_local):
            for upper in range(2):
                pltpu.make_async_copy(x_all.at[2, pl.ds((2 * e + upper) * cap, cap)], tok_ref.at[e, pl.ds(upper * (num_devs * cap // 2) + pair * cap, cap)], tok_sem).start()

    def fetch(n, cp, tp):
        return pltpu.make_async_copy(h_block(cp, tp), x_all.at[n % 2], load_sem.at[n % 2])

    for j in range(h_chunks // 2):
        diag(j)
    from_peer(4)
    across(4)
    await_bytes(h_block(r, near), h_near.at[OWN])
    fetch(1, r, near).start()
    fetch(1, r, near).wait()
    pick(0, ((me, hbuf), (r * tp_size + near, x_all.at[1])))
    for j in range(5, h_chunks):
        from_peer(j)
        across(j)
    fetch(0, peer, t).start()
    await_bytes(h_block(peer, near), h_near.at[PEER])
    fetch(1, peer, near).start()
    fetch(0, peer, t).wait()
    fetch(1, peer, near).wait()
    pick(1, ((peer * tp_size + t, x_all.at[0]), (peer * tp_size + near, x_all.at[1])))
    fetch(0, r, far).start()
    await_bytes(h_block(r, far_near), h_near.at[FAR])
    fetch(1, r, far_near).start()
    fetch(0, r, far).wait()
    fetch(1, r, far_near).wait()
    pick(2, ((r * tp_size + far, x_all.at[0]), (r * tp_size + far_near, x_all.at[1])))
    for j in range(4, h_chunks):
        diag(j)
    fetch(0, peer, far).start()
    await_bytes(h_block(peer, far_near), h_near.at[DIAG])
    fetch(1, peer, far_near).start()
    fetch(0, peer, far).wait()
    fetch(1, peer, far_near).wait()
    pick(3, ((peer * tp_size + far, x_all.at[0]), (peer * tp_size + far_near, x_all.at[1])))

    await_bytes(x_all.at[2], tok_sem)
    for n in range(2):
        await_bytes(part.at[n], near_send.at[n])
    await_bytes(h_ref.at[pl.ds(0, 7 * rows)], h_send)
    await_bytes(part.at[pl.ds(0, 2)], far_send)
    await_bytes(slots.at[pl.ds(0, num_devs - 1)], slot_send)
    await_bytes(x_all.at[pl.ds(0, 2)], x_send)
    await_bytes(kv_ref.at[pl.ds(0, tp_size * rows)], kv_send)


def moe_kernel(num_devs, tp_size, exp_local, cap, full, tok_ref, h_ref, slot_ref, slots_ref, gate_ref, wg_ref, wu_ref, wd_ref, y_ref, tok, wgb, wub, wdb, zrecv, over, cols, tsem, wsem, send_sem, over_sem, recv_sem):
    rows, width = y_ref.shape
    r, t = lax.axis_index('cp'), lax.axis_index('tp')
    me = r * tp_size + t
    near = t + 1 - 2 * lax.rem(t, 2)
    places = [(cp, lax.rem(tp + 2 * across, tp_size)) for across in range(2) for cp in (r, 1 - r) for tp in (t, near)]
    low = cap // 2
    pairs = exp_local // 2
    block = num_devs * cap
    half_block = block // 2

    def weight_copies(e, slot):
        return [pltpu.make_async_copy(src.at[e], dst.at[slot], wsem.at[i, slot]) for i, (src, dst) in enumerate(((wg_ref, wgb), (wu_ref, wub), (wd_ref, wdb)))]

    loads = [pltpu.make_async_copy(tok_ref.at[at], tok.at[at], tsem.at[n]) for n, at in enumerate((pl.ds(0, 2), pl.ds(2, exp_local - 2)))]
    for e in range(2):
        loads[e].start()
        for copy in weight_copies(e, e):
            copy.start()
    greet(places[1:])
    slot = slot_ref[0:2, :]
    pos = slot % cap
    expert = slot // cap
    dev = expert // exp_local
    el = expert % exp_local
    dev_cp, dev_tp = dev // tp_size, dev % tp_size
    place = jnp.where(dev_tp % 2 == t % 2, 0, 1) + jnp.where(dev_cp == r, 0, 2) + jnp.where(dev_tp // 2 == t // 2, 0, 4)
    home = (el // 2) * block + place * cap + (el % 2) * low + pos % low
    upper = pairs * block + (home if full else place * OV + slot_ref[2:4, :])
    back = jnp.where(pos < low, home, upper)
    columns = jnp.concatenate([back.astype(jnp.float32), gate_ref[...], jnp.zeros((124, rows), jnp.float32)], axis=0)
    cols[...] = jnp.transpose(columns)
    y_ref[...] = h_ref[...].astype(jnp.float32)
    loads[0].wait()

    def send(src, dst, sem, group, n):
        rdma(src, dst, sem, recv_sem.at[group], *places[n]).start()

    def two_experts(m, carry):
        @pl.when(m == 1)
        def _():
            loads[1].wait()

        outs = []
        for b in range(2):
            e = 2 * m + b
            for copy in weight_copies(e, b):
                copy.wait()
            x = tok[e]
            gate = jnp.dot(x, wgb[b], preferred_element_type=jnp.float32)
            up = jnp.dot(x, wub[b], preferred_element_type=jnp.float32)
            act = (jax.nn.silu(gate) * up).astype(jnp.bfloat16)
            outs.append(jnp.dot(act, wdb[b], preferred_element_type=jnp.float32))

            @pl.when(e + 2 < exp_local)
            def _():
                for copy in weight_copies(e + 2, b):
                    copy.start()

        for side in range(2):
            pieces = [z[side * half_block:(side + 1) * half_block].reshape(num_devs, low, width) for z in outs]
            tok[2 * m + side] = jnp.concatenate(pieces, axis=1).reshape(block, width).astype(jnp.bfloat16)
            if side == 0 or full:
                at = side * pairs + m
                for n in range(1, num_devs):
                    part = pl.ds(n * cap, cap)
                    send(tok.at[2 * m + side, part], zrecv.at[at, part], over_sem if side else send_sem, at // 2, n)
                zrecv[at, :cap, :] = tok[2 * m + side, :cap, :]
        return carry

    lax.fori_loop(0, pairs, two_experts, 0)

    if not full:
        per_block = block // OV
        for n in (4, 5, 6, 7, 2, 3, 1, 0):
            cp, tp = places[n]
            ids = slots_ref[cp * tp_size + tp]
            mix = jnp.zeros((OV, half_block), jnp.float32)
            for k in range(2):
                own = ids[k:k + 1, :] - me * exp_local * cap
                inside = jnp.logical_and(own >= 0, own < exp_local * cap)
                spot = jnp.where(jnp.logical_and(inside, own % cap >= low), own // cap * low + own % cap - low, -1)
                a = jnp.where(ids[2 + k:3 + k, :] == lax.broadcasted_iota(jnp.int32, (OV, rows), 0), 1.0, 0.0).astype(jnp.bfloat16)
                b = jnp.where(spot == lax.broadcasted_iota(jnp.int32, (half_block * 2, rows), 0), 1.0, 0.0).astype(jnp.bfloat16)
                mix = lax.dot_general(a, b, (((1,), (1,)), ((), ())), preferred_element_type=jnp.float32) + (mix if k else 0.0)
            mix = mix.astype(jnp.bfloat16)
            for c0 in range(0, width, 512):
                z = jnp.concatenate([tok[2 * m + 1, n * cap:(n + 1) * cap, c0:c0 + 512] for m in range(pairs)], axis=0)
                over[n, :, c0:c0 + 512] = jnp.dot(mix, z, preferred_element_type=jnp.float32).astype(jnp.bfloat16)
            dst = zrecv.at[pairs + n // per_block, pl.ds(n % per_block * OV, OV)]
            if n:
                send(over.at[n], dst, over_sem, pairs // 2, n)
            else:
                dst[...] = over[n]

    groups = recv_sem.shape[0]
    span = 2 * block

    def combine(g, carry):
        await_bytes(zrecv.at[pl.ds(0, 2), pl.ds(0, (num_devs - 1) * cap)], recv_sem.at[g])
        want = (lax.broadcasted_iota(jnp.int32, (rows, span), 1) + g * span).astype(jnp.float32)
        sel0 = jnp.where(cols[:, 0:1] == want, 1.0, 0.0).astype(jnp.bfloat16)
        sel1 = jnp.where(cols[:, 1:2] == want, 1.0, 0.0).astype(jnp.bfloat16)
        first = pl.multiple_of(g * 2, 2)
        for c0 in range(0, width, 512):
            z = zrecv[pl.ds(first, 2), :, c0:c0 + 512].reshape(span, 512)
            z0 = jnp.dot(sel0, z, preferred_element_type=jnp.float32)
            z1 = jnp.dot(sel1, z, preferred_element_type=jnp.float32)
            y_ref[:, c0:c0 + 512] += cols[:, 2:3] * z0 + cols[:, 3:4] * z1
        return carry

    lax.fori_loop(0, groups, combine, 0)
    await_bytes(tok.at[pl.ds(0, pairs), pl.ds(0, (num_devs - 1) * cap)], send_sem)
    await_bytes(tok.at[pl.ds(0, pairs if full else 2), pl.ds(0, (num_devs - 1) * cap)], over_sem)


def solution(mesh):
    cp_size = mesh.shape['cp']
    tp_size = mesh.shape['tp']
    num_devs = cp_size * tp_size
    row_spec = P(('data', 'cp', 'tp'), None)
    head_spec = P(None, 'tp', None)
    wo_spec = P('tp', None, None)
    expert_spec = P(('cp', 'tp'), None, None)

    vmem = pl.BlockSpec(memory_space=pltpu.VMEM)
    hbm = pl.BlockSpec(memory_space=pl.ANY)
    dma = pltpu.SemaphoreType.DMA
    bf16, f32 = jnp.bfloat16, jnp.float32

    def params(number):
        return pltpu.CompilerParams(collective_id=number, has_side_effects=True, vmem_limit_bytes=VLIM)

    def front(x_blk, idx, w_q, w_k, w_v, w_o, heads, hd, exp_local, cap):
        rows, width = x_blk.shape
        group = rows * tp_size
        v32 = lambda *shape: pltpu.VMEM(shape, f32)
        v16 = lambda *shape: pltpu.VMEM(shape, bf16)
        return pl.pallas_call(
            functools.partial(front_kernel, cp_size, tp_size, heads, hd, exp_local * num_devs, cap),
            in_specs=[vmem, vmem, hbm, hbm, hbm, hbm],
            out_specs=[hbm, hbm, vmem, vmem, vmem],
            out_shape=[jax.ShapeDtypeStruct((rows * num_devs, width), bf16), jax.ShapeDtypeStruct((exp_local, num_devs * cap, width), bf16), jax.ShapeDtypeStruct((rows, width), bf16), jax.ShapeDtypeStruct((8, rows), jnp.int32), jax.ShapeDtypeStruct((num_devs, 8, rows), jnp.int32)],
            scratch_shapes=[
                v16(3, rows, width), v16(width, heads * hd), v16(width, 2 * hd), v16(heads * hd, width), v16(group, heads * hd), v16(group * cp_size, 2 * hd),
                v32(heads * QB, 128), v32(heads * QB, 128), v32(heads * QB, hd), v16(QB, heads * hd),
                v32(6, QB, width), v32(4, QB, width), v32(2, QB, width),
                dma((3,)), dma, dma, dma, dma, dma((rows // CH,)), dma, dma((rows // CH,)), dma, dma((2,)),
                dma((2,)), dma((4,)), dma, dma((2, QB // CH)), dma, dma((4,)), dma((rows // HC,)), dma((rows // HC,)), dma((rows // HC,)), dma((2,)), dma, v16(2, WR, heads, hd), dma((2,))],
            compiler_params=params(0),
            name='front',
        )(x_blk, idx, w_q, w_k, w_v, w_o)

    def experts(full, cap, tok, h_own, own_slots, slots, gates, w_gate, w_up, w_down):
        rows, width = h_own.shape
        exp_local, _, ff = w_gate.shape
        v16 = lambda *shape: pltpu.VMEM(shape, bf16)
        block = num_devs * cap
        blocks = exp_local if full else exp_local // 2 + num_devs * OV // block
        return pl.pallas_call(
            functools.partial(moe_kernel, num_devs, tp_size, exp_local, cap, full),
            in_specs=[hbm, vmem, vmem, vmem, vmem, hbm, hbm, hbm],
            out_specs=vmem,
            out_shape=jax.ShapeDtypeStruct((rows, width), f32),
            scratch_shapes=[v16(exp_local, block, width), v16(2, width, ff), v16(2, width, ff), v16(2, ff, width), v16(blocks, block, width), v16(num_devs, OV, width), pltpu.VMEM((rows, 128), f32), dma((2,)), dma((3, 2)), dma, dma, dma((blocks // 2,))],
            compiler_params=params(2 if full else 1),
            name='moe_full' if full else 'moe',
        )(tok, h_own, own_slots, slots, gates, w_gate, w_up, w_down)

    def device_fn(x_blk, w_q, w_k, w_v, w_o, idx_blk, gate_blk, w_gate, w_up, w_down):
        tok_dev, width = x_blk.shape
        heads, head_dim = w_q.shape[1], w_k.shape[2]
        exp_local = w_gate.shape[0]
        num_exp = exp_local * num_devs
        capacity = 4 * tok_dev // num_exp

        flat = lambda w: w.reshape(width, -1)
        _, tok, h_own, own_slots, slots = front(x_blk, idx_blk.T, w_q, flat(w_k), flat(w_v), w_o.reshape(heads * head_dim, width), heads, head_dim, exp_local, capacity)
        few = jnp.max(slots[:, 4, 0]) <= LIMIT
        total = lax.cond(few, functools.partial(experts, False, capacity), functools.partial(experts, True, capacity), tok, h_own, own_slots, slots, gate_blk.T, w_gate, w_up, w_down)
        return total.astype(bf16)

    return jax.shard_map(device_fn, mesh=mesh, in_specs=(row_spec, head_spec, head_spec, head_spec, wo_spec, row_spec, row_spec, expert_spec, expert_spec, expert_spec), out_specs=row_spec, check_vma=False)
```
